128 devices in a mesh: frame: 32 (over x, y, z_lo), row: 4 (over z_hi, core).
Axes of the slice: x: 4, y: 4, z: 4 (z_hi: 2, z_lo: 2; z = z_hi * 2 + z_lo), core: 2. Of those that a mesh axis runs over, the one named last changes fastest.
Arguments:
- tokens: bfloat16 [32, 512, 2048], P('frame', 'row'), may hold values from -6 to 6
- w_gate: bfloat16 [2048, 4096], P(None, 'row'), may hold values from -0.125 to 0.125
- w_value: bfloat16 [2048, 4096], P(None, 'row'), may hold values from -0.125 to 0.125
- w_state_proj: bfloat16 [2048, 512], replicated, may hold values from -0.03125 to 0.03125
- w_step: bfloat16 [2, 2048, 64], P(None, None, 'row'), may hold values from -0.125 to 0.125
- step_bias: float32 [2, 64], P(None, 'row'), may hold values from -3 to 0
- decay_rate: float32 [2, 64], P(None, 'row'), may hold values from 0 to 0.3, as said below
- conv_taps: float32 [2, 4, 4096], P(None, None, 'row'), may hold values from -3 to 3
- skip_gain: float32 [2, 64], P(None, 'row'), may hold values from 0.1 to 16, as said below
- norm_gain: float32 [4096], P('row'), may hold values from 0.1 to 1.9
- w_out: bfloat16 [4096, 2048], P('row'), may hold values from -0.09375 to 0.09375
Outputs:
- mixed: bfloat16 [32, 512, 2048], P('frame', 'row')
The draws below stay inside these ranges and needn't reach their ends.
Inputs may be any that keep to these rules, and one draw needn't show every extreme that they name: `decay_rate`: positive decay rates. `skip_gain`: positive skip weights.
All inputs are finite; a program needn't handle non-finite values.
Results may differ from the reference program's by a relative error of at most 0.015.
Values may be sent and summed in bfloat16 or wider, within the bound.
A program may use at most 128 MiB of HBM per device.

```python
import jax
import jax.numpy as jnp
from jax import lax

D = 2048
D_INNER = 4096
HEADS = 64
HEAD_DIM = 64
STATE = 128
PATCHES = 512
CONV = 4
BLK = 128
FRAMES = 32


def draw_decay_rate(key, part):
    first, second, third = jax.random.split(jax.random.fold_in(key, 7), 3)
    share = 0.5
    quick_mask = jax.random.uniform(first, (2, HEADS)) < share
    slow_rate = jnp.exp(jax.random.uniform(second, (2, HEADS), minval=jnp.log(0.5), maxval=jnp.log(2.0))) / (0.4 * FRAMES * PATCHES)
    quick_rate = jnp.exp(jax.random.uniform(third, (2, HEADS), minval=jnp.log(0.05), maxval=jnp.log(0.3)))
    return jnp.where(quick_mask, quick_rate, slow_rate).astype(jnp.float32)


def draw_skip_gain(key, part):
    second = jax.random.fold_in(jax.random.fold_in(key, 11), 1)
    value = jnp.exp(jax.random.uniform(second, (2, HEADS), minval=jnp.log(0.25), maxval=jnp.log(8.0)))
    return value.astype(jnp.float32)


def levels(own_key, shape, pieces, least, largest):
    factor_of, own = 1.0, jax.random.fold_in(own_key, 6)
    for axis_at, parts in pieces:
        heights = jnp.exp(jax.random.uniform(jax.random.fold_in(own, axis_at), (parts,), jnp.float32, least / len(pieces), largest / len(pieces)))
        factor_of = factor_of * jnp.repeat(heights, shape[axis_at] // parts).reshape([-1 if axis == axis_at else 1 for axis in range(len(shape))])
    return factor_of


def normal_values(key, extent, scale, most, cuts=(), dtype=jnp.bfloat16):
    loudness = levels(key, extent, cuts, -0.22, 0.18) if cuts else 1.0
    values = jax.random.normal(key, extent, jnp.float32) * scale * loudness
    return jnp.minimum(jnp.maximum(values, -most), most).astype(dtype)


def setup_inputs(seed: int = 0) -> dict:
    splits = jax.random.split(jax.random.key(seed), 12)
    return {
        "tokens": normal_values(splits[0], (FRAMES, PATCHES, D), 1.0, 6.0, ((0, 32), (1, 4))),
        "w_gate": normal_values(splits[1], (D, D_INNER), D ** -0.5, 0.125, ((1, 4),)),
        "w_value": normal_values(splits[2], (D, D_INNER), D ** -0.5, 0.125, ((1, 4),)),
        "w_state_proj": normal_values(splits[3], (D, 4 * STATE), (16 * D) ** -0.5, 0.03125),
        "w_step": normal_values(splits[4], (2, D, HEADS), D ** -0.5, 0.125, ((2, 4),)),
        "step_bias": jnp.clip(-3.0 + 3.0 * jax.random.uniform(splits[5], (2, HEADS), jnp.float32) ** levels(splits[5], (2, HEADS), ((1, 4),), -0.2, 0.2), -3.0, 0.0),
        "decay_rate": draw_decay_rate(jax.random.fold_in(splits[11], 71), 0),
        "conv_taps": normal_values(splits[7], (2, CONV, D_INNER), CONV ** -0.5, 3.0, ((2, 4),), jnp.float32),
        "skip_gain": draw_skip_gain(jax.random.fold_in(splits[11], 71), 0),
        "norm_gain": jnp.clip(1.0 + 0.18 * jax.random.normal(splits[9], (D_INNER,), jnp.float32), 0.1, 1.9),
        "w_out": normal_values(splits[10], (D_INNER, D), D_INNER ** -0.5, 0.09375, ((0, 4),)),
    }


def block_weights(scores, log_cum, dt_block):
    size = scores.shape[0]
    row_index = lax.broadcasted_iota(jnp.int32, (size, size), 0)
    col_index = lax.broadcasted_iota(jnp.int32, (size, size), 1)
    causal = row_index >= col_index
    log_gap = log_cum.T[:, :, None] - log_cum.T[:, None, :]
    fading = jnp.exp(jnp.where(causal[None], log_gap, -jnp.inf))
    return (scores[None] * fading * dt_block.T[:, None, :]).astype(jnp.bfloat16)

def scan_direction(values, b_rows, c_rows, dt_rows, rate_row, skip_row):
    tok_count = values.shape[0]
    block_count = tok_count // BLK
    blocks = (values.reshape(block_count, BLK, HEADS, HEAD_DIM), b_rows.reshape(block_count, BLK, STATE), c_rows.reshape(block_count, BLK, STATE), dt_rows.reshape(block_count, BLK, HEADS))

    def advance(carry_state, block):
        x_block, b_block, c_block, dt_block = block
        log_cum = jnp.cumsum(-dt_block * rate_row[None, :], axis=0)
        scores = jnp.dot(c_block, b_block.T, preferred_element_type=jnp.float32)
        weights = block_weights(scores, log_cum, dt_block)
        x_wide = x_block.astype(jnp.float32)
        inner_out = jnp.einsum('hts,shp->thp', weights.astype(jnp.float32), x_wide)
        state_b = carry_state.astype(jnp.bfloat16)
        carried_out = jnp.einsum('tn,hpn->thp', c_block.astype(jnp.float32), state_b.astype(jnp.float32))
        result = inner_out + carried_out * jnp.exp(log_cum)[:, :, None] + skip_row[None, :, None] * x_wide
        log_last = log_cum[-1]
        carried = ((jnp.exp(log_last[None, :] - log_cum) * dt_block)[:, :, None] * x_wide).astype(jnp.bfloat16)
        update = jnp.einsum('sn,shp->hpn', b_block.astype(jnp.float32), carried.astype(jnp.float32))
        return (jnp.exp(log_last)[:, None, None] * carry_state + update, result)
    state_zero = jnp.zeros((HEADS, HEAD_DIM, STATE), jnp.float32)
    unused_state, outputs = lax.scan(advance, state_zero, blocks)
    return outputs.reshape(tok_count, HEADS, HEAD_DIM)

def conv_pass(padded, taps, tok_count, backward):
    reach = taps.shape[0] - 1
    running = jnp.zeros((tok_count, padded.shape[1]), jnp.float32)
    for tap_index in range(taps.shape[0]):
        first_row = 2 * reach - tap_index if backward else tap_index
        running = running + taps[tap_index][None, :] * padded[first_row:first_row + tok_count]
    return jax.nn.silu(running).astype(jnp.bfloat16)

def reference(tokens, w_gate, w_value, w_state_proj, w_step, step_bias, decay_rate, conv_taps, skip_gain, norm_gain, w_out):
    tok_count = FRAMES * PATCHES
    flat = tokens.reshape(tok_count, D)

    def project(matrix):
        return jnp.dot(flat, matrix, preferred_element_type=jnp.float32).astype(jnp.bfloat16)
    gate_in = project(w_gate)
    x_raw = project(w_value)
    bc_cols = project(w_state_proj)
    dt_forward = jax.nn.softplus(project(w_step[0]).astype(jnp.float32) + step_bias[0][None, :])
    dt_backward = jax.nn.softplus(project(w_step[1]).astype(jnp.float32) + step_bias[1][None, :])
    padded = jnp.pad(x_raw.astype(jnp.float32), ((CONV - 1, CONV - 1), (0, 0)))
    x_forward = conv_pass(padded, conv_taps[0], tok_count, False).reshape(tok_count, HEADS, HEAD_DIM)
    x_backward = conv_pass(padded, conv_taps[1], tok_count, True).reshape(tok_count, HEADS, HEAD_DIM)
    y_forward = scan_direction(x_forward, bc_cols[:, :STATE], bc_cols[:, STATE:2 * STATE], dt_forward, decay_rate[0], skip_gain[0])
    y_backward = jnp.flip(scan_direction(jnp.flip(x_backward, 0), jnp.flip(bc_cols[:, 2 * STATE:3 * STATE], 0), jnp.flip(bc_cols[:, 3 * STATE:], 0), jnp.flip(dt_backward, 0), decay_rate[1], skip_gain[1]), 0)
    summed = (y_forward + y_backward).reshape(tok_count, D_INNER)
    gated = summed * jax.nn.silu(gate_in.astype(jnp.float32))
    scale = lax.rsqrt(lax.optimization_barrier(jnp.mean(gated * gated, axis=-1, keepdims=True)) + 1e-05)
    normed = (gated * scale * norm_gain[None, :]).astype(jnp.bfloat16)
    mixed = jnp.dot(normed, w_out, preferred_element_type=jnp.float32).astype(jnp.bfloat16)
    return mixed.reshape(FRAMES, PATCHES, D)
```

```python
import jax
import jax.numpy as jnp
from jax import lax
from jax.experimental import pallas as pl
from jax.experimental.pallas import tpu as pltpu
from jax.sharding import PartitionSpec as P

BF = jnp.bfloat16
F32 = jnp.float32
FRAMES = 32
TOK = 512
BLK = 128
NBLK = 4
CH = 1024
D = 2048
HALF = 256
HALO = 8
LOG2E = 1.4426950408889634
D_INNER = 4096
VM = pl.BlockSpec(memory_space=pltpu.VMEM)
ANY = pl.BlockSpec(memory_space=pl.ANY)
MSG = 72


def silu(x):
    return 0.5 * x * (1.0 + jnp.tanh(0.5 * x))


def dot(a, b):
    return jnp.dot(a, b, preferred_element_type=F32)


def dev(frame, row):
    return {"frame": frame, "row": row}


def place():
    frame, row = lax.axis_index("frame"), lax.axis_index("row")
    core = lax.rem(row, 2)
    return frame, row, core, lax.div(row, 2)


def remote(src, dst, send, recv, target):
    return pltpu.make_async_remote_copy(src, dst, send, recv, device_id=target)


CHUNKS = 4
CROWS = 128 // CHUNKS


def project_body(
    tok_ref, wg_ref, wv_ref, ws_ref, wt_ref,
    gate_ref, xr_ref, halo_ref, bc_ref, st_ref,
    tb, wg, wv, ws, wt, wc, w_sem, s_sem, r_sem,
):
    frame, row, core, hi = place()
    partner = row + 1 - 2 * core
    across = lax.rem(row + 2, 4)
    loads = []
    for i, (src, dst) in enumerate(((wv_ref, wv), (wg_ref, wg), (ws_ref, ws), (wt_ref, wt))):
        copy = pltpu.make_async_copy(src, dst, w_sem.at[i])
        copy.start()
        loads.append(copy)

    barrier = pltpu.get_barrier_semaphore()
    first, final = frame == 0, frame == FRAMES - 1
    for peer in (partner, across):
        pl.semaphore_signal(barrier, inc=1, device_id=dev(frame, peer))

    @pl.when(jnp.logical_not(first))
    def _():
        pl.semaphore_signal(barrier, inc=1, device_id=dev(frame - 1, 3))

    @pl.when(jnp.logical_not(final))
    def _():
        pl.semaphore_signal(barrier, inc=1, device_id=dev(frame + 1, 0))

    to_next = jnp.logical_and(row == 3, jnp.logical_not(final))
    to_prev = jnp.logical_and(row == 0, jnp.logical_not(first))
    pl.semaphore_wait(barrier, jnp.where(jnp.logical_or(to_next, to_prev), 6, 2))

    cross, local = [], []
    for i in range(CHUNKS):
        rows = pl.ds(i * CROWS, CROWS)
        copy = remote(
            tok_ref.at[rows],
            tb.at[pl.ds(HALF + 16 + core * 128 + i * CROWS, CROWS)],
            s_sem.at[i], r_sem.at[i], dev(frame, across),
        )
        copy.start()
        cross.append(copy)
    mine = remote(
        tok_ref, tb.at[pl.ds(core * 128, 128)], s_sem.at[CHUNKS], r_sem.at[CHUNKS],
        dev(frame, partner),
    )
    mine.start()

    def halo_copies(up):
        src = tok_ref.at[pl.ds(128 - HALO if up else 0, HALO)]
        dst = tb.at[pl.ds(HALF + (0 if up else HALO), HALO)]
        base = 2 * CHUNKS + 1 + (0 if up else 4)
        return [
            remote(
                src, dst, s_sem.at[base + r], r_sem.at[2 * CHUNKS + 1 + (0 if up else 1)],
                dev(frame + 1 if up else frame - 1, r),
            )
            for r in range(4)
        ]

    for up, flag in ((True, to_next), (False, to_prev)):

        @pl.when(flag)
        def _(up=up):
            for copy in halo_copies(up):
                copy.start()

    tb[pl.ds(core * 128, 128), :] = tok_ref[...]
    for up, flag in ((True, first), (False, final)):

        @pl.when(flag)
        def _(up=up):
            tb[pl.ds(HALF + (0 if up else HALO), HALO), :] = jnp.zeros((HALO, D), BF)

    def multiply(lo, count, put):
        def over(weight, columns, width, store):
            @pl.loop(0, columns // width)
            def _(n):
                cols = pl.ds(pl.multiple_of(n * width, width), width)
                out = dot(tb[lo : lo + count, :], weight[:, cols]).astype(BF)
                store(out, cols)

        return over

    def phase(lo, count, skip, base, waits):
        over = multiply(lo, count, None)
        rows = pl.ds(pl.multiple_of(base, HALF), HALF)

        def put(ref):
            def store(out, cols):
                ref[rows, cols] = out[skip:]

            return store

        def put_value(out, cols):
            xr_ref[rows, cols] = out[skip:]
            if skip:
                halo_ref[:, cols] = out[:skip]

        if waits:
            loads[0].wait()
        over(wv, CH, 256, put_value)
        if waits:
            loads[1].wait()
        over(wg, CH, 256, put(gate_ref))
        if waits:
            loads[2].wait()
            loads[3].wait()
            wc[...] = jnp.zeros_like(wc)
            wc[:, 0:16] = wt[0]
            wc[:, 16:32] = wt[1]
        over(ws, 512, 256, put(bc_ref))
        over(wc, 128, 128, put(st_ref))

    mine.wait_recv()
    phase(0, HALF, 0, hi * HALF, True)

    for i in range(CHUNKS):
        cross[i].wait_recv()
        rows = pl.ds(HALF + 16 + core * 128 + i * CROWS, CROWS)
        copy = remote(
            tb.at[rows], tb.at[rows], s_sem.at[CHUNKS + 1 + i], r_sem.at[CHUNKS + 1 + i],
            dev(frame, partner),
        )
        copy.start()
        local.append(copy)
    for up, flag in ((True, first), (False, final)):

        @pl.when(jnp.logical_not(flag))
        def _(up=up):
            halo_copies(up)[0].wait_recv()

    for copy in local:
        copy.wait_recv()
    phase(HALF, HALF + 16, 16, (1 - hi) * HALF, False)
    mine.wait_send()
    for copy in cross + local:
        copy.wait_send()
    for up, flag in ((True, to_next), (False, to_prev)):

        @pl.when(flag)
        def _(up=up):
            for copy in halo_copies(up):
                copy.wait_send()


def project(tokens, w_gate, w_value, w_state, w_step):
    sds = jax.ShapeDtypeStruct
    return pl.pallas_call(
        project_body,
        name="project",
        out_shape=(
            sds((TOK, CH), BF), sds((TOK, CH), BF), sds((16, CH), BF),
            sds((TOK, 512), BF), sds((TOK, 128), BF),
        ),
        in_specs=[VM, ANY, ANY, ANY, ANY],
        out_specs=(VM,) * 5,
        scratch_shapes=[
            pltpu.VMEM((HALF + 16 + HALF, D), BF),
            pltpu.VMEM((D, CH), BF), pltpu.VMEM((D, CH), BF), pltpu.VMEM((D, 512), BF),
            pltpu.VMEM((2, D, 16), BF), pltpu.VMEM((D, 128), BF),
            pltpu.SemaphoreType.DMA((4,)),
            pltpu.SemaphoreType.DMA((2 * CHUNKS + 1 + 8,)),
            pltpu.SemaphoreType.DMA((2 * CHUNKS + 3,)),
        ],
        compiler_params=pltpu.CompilerParams(
            collective_id=0, has_side_effects=True, vmem_limit_bytes=60 * 1024 * 1024
        ),
    )(tokens, w_gate, w_value, w_state, w_step)


def expand(values, base):
    lane = lax.broadcasted_iota(jnp.int32, (1, 128), 1)
    return jnp.where(lane < 64, values[:, base : base + 1], values[:, base + 1 : base + 2])


def lanes(group):
    return slice(group * 128, group * 128 + 128)


def scan_body(
    xr_ref, halo_ref, bc_ref, st_ref, par_ref, taps_ref,
    msg_ref, y_ref, ef_ref,
    xp, xs, xdt, start, state, car, cum_s, dt_s, tot_s,
):
    row_i = lax.broadcasted_iota(jnp.int32, (BLK, BLK), 0)
    col_i = lax.broadcasted_iota(jnp.int32, (BLK, BLK), 1)
    lower = (row_i >= col_i)
    forward = col_i < 16
    xp[0:8, :] = halo_ref[0:8, :].astype(F32)
    xp[8 : 8 + TOK, :] = xr_ref[...].astype(F32)
    xp[8 + TOK :, :] = halo_ref[8:16, :].astype(F32)
    bias, rate = par_ref[0:1, :], par_ref[1:2, :] * LOG2E
    raw = st_ref[...].astype(F32) + bias
    dt = jnp.maximum(raw, 0.0) + jnp.log1p(jnp.exp(-jnp.abs(raw)))
    dt_s[...] = dt
    step = -dt * rate
    tri = lower.astype(BF)
    totals = []
    for j in range(NBLK):
        part = step[j * BLK : (j + 1) * BLK]
        high = part.astype(BF)
        rest = part - high.astype(F32)
        mid = rest.astype(BF)
        low = (rest - mid.astype(F32)).astype(BF)
        cum = dot(tri, high) + (dot(tri, mid) + dot(tri, low))
        total = cum[BLK - 1 : BLK]
        cum_s[j * BLK : (j + 1) * BLK] = jnp.where(forward, cum, (total - cum) + part)
        totals.append(total)
    zero = jnp.zeros((1, 128), F32)
    before, after = [zero], [zero]
    for j in range(NBLK - 1):
        before.append(before[-1] + totals[j])
        after.append(after[-1] + totals[NBLK - 1 - j])
    after = after[::-1]
    forward1 = forward[0:1]
    for j in range(NBLK):
        rows = slice(j * BLK, (j + 1) * BLK)
        ef_ref[rows] = jnp.exp2(cum_s[rows] + jnp.where(forward1, before[j], after[j]))
        tot_s[j : j + 1] = totals[j]
    whole = before[-1] + totals[-1]

    @pl.loop(0, NBLK)
    def _(j):
        for g in range(8):
            window = xp[pl.ds(pl.multiple_of(j * BLK, BLK), BLK + 16), lanes(g)]
            shifted = {
                o: pltpu.roll(window, (-o) % (BLK + 16), 0)[8 : 8 + BLK] for o in range(-3, 4)
            }
            for d in range(2):
                acc = None
                for k in range(4):
                    term = taps_ref[d, k : k + 1, lanes(g)] * shifted[3 - k if d else k - 3]
                    acc = term if acc is None else acc + term
                xs[d, pl.ds(pl.multiple_of(j * BLK, BLK), BLK), lanes(g)] = silu(acc).astype(BF)

    state[...] = jnp.zeros_like(state)

    @pl.loop(0, NBLK)
    def _(i):
        for d in range(2):
            j = i if d == 0 else NBLK - 1 - i
            rows = pl.ds(pl.multiple_of(j * BLK, BLK), BLK)
            total = tot_s[pl.ds(j, 1)]
            dt_j = dt_s[rows]
            fade = jnp.exp2(total - cum_s[rows]) * dt_j
            kept = jnp.exp2(total)
            for g in range(8):
                x = xs[d, rows, lanes(g)].astype(F32)
                car[:, lanes(g)] = (x * expand(fade, d * 16 + 2 * g)).astype(BF)
                xdt[d, rows, lanes(g)] = (x * expand(dt_j, d * 16 + 2 * g)).astype(BF)
            b = bc_ref[rows, d * 256 : d * 256 + 128]
            bt = b.astype(F32).T.astype(BF)
            for g in range(8):
                old = state[d, :, lanes(g)]
                start[d, pl.ds(j, 1), :, lanes(g)] = old.astype(BF)[None]
                state[d, :, lanes(g)] = (
                    old * expand(kept, d * 16 + 2 * g) + dot(bt, car[:, lanes(g)])
                )

    row8 = lax.broadcasted_iota(jnp.int32, (8, 128), 0)
    shrink = jnp.exp2(whole)
    for g in range(8):
        decay = [expand(shrink, d * 16 + 2 * g) for d in range(2)]
        high = [v.astype(BF).astype(F32) for v in decay]
        tail = jnp.zeros((8, 128), F32)
        for k, v in enumerate((high[0], decay[0] - high[0], high[1], decay[1] - high[1])):
            tail = jnp.where(row8 == k, v, tail)
        for r in range(4):
            piece = g * 4 + r
            for d in range(2):
                msg_ref[piece, d * 32 : d * 32 + 32] = state[
                    d, r * 32 : r * 32 + 32, lanes(g)
                ].astype(BF)
            msg_ref[piece, 64:72] = tail.astype(BF)

    skip = par_ref[2:3, :]
    upper = col_i >= row_i

    @pl.loop(0, NBLK)
    def _(j):
        rows = pl.ds(pl.multiple_of(j * BLK, BLK), BLK)
        cum = cum_s[rows]
        cum_t = cum.T
        grown = jnp.exp2(cum)
        c, scores = [], []
        for d in range(2):
            b = bc_ref[rows, d * 256 : d * 256 + 128]
            c.append(bc_ref[rows, d * 256 + 128 : d * 256 + 256])
            s = lax.dot_general(
                c[d], b, (((1,), (1,)), ((), ())), preferred_element_type=F32
            )
            scores.append(jnp.where(lower if d == 0 else upper, s, 0.0))
        for g in range(8):
            values = jnp.concatenate([xdt[0, rows, lanes(g)], xdt[1, rows, lanes(g)]], axis=0)
            outs = []
            for k in range(2):
                h = 2 * g + k
                w = []
                for d in range(2):
                    n = d * 16 + h
                    gap = jnp.minimum(cum[:, n : n + 1] - cum_t[n : n + 1, :], 0.0)
                    w.append((scores[d] * jnp.exp2(gap)).astype(BF))
                outs.append(dot(jnp.concatenate(w, axis=1), values))
            y = jnp.where(col_i < 64, outs[0], outs[1])
            for d in range(2):
                carried = dot(c[d], start[d, j, :, lanes(g)])
                y = y + expand(grown, d * 16 + 2 * g) * carried
                y = y + expand(skip, d * 16 + 2 * g) * xs[d, rows, lanes(g)].astype(F32)
            y_ref[rows, lanes(g)] = y


def local_scan(x_raw, halo, bc, step, params, taps):
    sds = jax.ShapeDtypeStruct
    return pl.pallas_call(
        scan_body,
        name="local_scan",
        out_shape=(sds((32, MSG, 128), BF), sds((TOK, CH), F32), sds((TOK, 128), F32)),
        in_specs=[VM] * 6,
        out_specs=(VM,) * 3,
        scratch_shapes=[
            pltpu.VMEM((TOK + 16, CH), F32),
            pltpu.VMEM((2, TOK, CH), BF),
            pltpu.VMEM((2, TOK, CH), BF),
            pltpu.VMEM((2, NBLK, 128, CH), BF),
            pltpu.VMEM((2, 128, CH), F32),
            pltpu.VMEM((BLK, CH), BF),
            pltpu.VMEM((TOK, 128), F32),
            pltpu.VMEM((TOK, 128), F32),
            pltpu.VMEM((8, 128), F32),
        ],
        compiler_params=pltpu.CompilerParams(vmem_limit_bytes=60 * 1024 * 1024),
    )(x_raw, halo, bc, step, params, taps)


def states_body(msg_ref, inc_ref, got, out, back, s_sem, r_sem, s2_sem, r2_sem):
    frame, row, core, hi = place()
    barrier = pltpu.get_barrier_semaphore()
    peers = [lax.rem(frame + i, FRAMES) for i in range(1, FRAMES)]
    for peer in peers:
        pl.semaphore_signal(barrier, inc=1, device_id=dev(peer, row))
    pl.semaphore_wait(barrier, FRAMES - 1)
    copies = []
    for i, peer in enumerate(peers):
        copy = remote(msg_ref.at[peer], got.at[frame], s_sem.at[i], r_sem.at[i], dev(peer, row))
        copy.start()
        copies.append(copy)
    got[frame] = msg_ref[frame]
    for copy in copies:
        copy.wait_recv()
    for d in range(2):
        state = jnp.zeros((32, 128), F32)
        for g in range(FRAMES) if d == 0 else reversed(range(FRAMES)):
            out[g, d * 32 : d * 32 + 32] = state.astype(BF)
            tail = got[g, 64:72].astype(F32)
            decay = tail[2 * d : 2 * d + 1] + tail[2 * d + 1 : 2 * d + 2]
            state = decay * state + got[g, d * 32 : d * 32 + 32].astype(F32)
    returns = []
    for i, peer in enumerate(peers):
        copy = remote(out.at[peer], back.at[frame], s2_sem.at[i], r2_sem.at[i], dev(peer, row))
        copy.start()
        returns.append(copy)
    back[frame] = out[frame]
    for copy in returns:
        copy.wait_recv()
    inc_ref[...] = back[...]
    for copy in copies + returns:
        copy.wait_send()


def exchange(msg):
    return pl.pallas_call(
        states_body,
        name="states",
        out_shape=jax.ShapeDtypeStruct((32, 64, 128), BF),
        in_specs=[VM],
        out_specs=VM,
        scratch_shapes=[
            pltpu.VMEM((32, MSG, 128), BF),
            pltpu.VMEM((32, 64, 128), BF),
            pltpu.VMEM((32, 64, 128), BF),
        ]
        + [pltpu.SemaphoreType.DMA((31,))] * 4,
        compiler_params=pltpu.CompilerParams(collective_id=1, has_side_effects=True),
    )(msg)


COLS = 512
NCOL = D // COLS


def finish_body(
    y_ref, gate_ref, bc_ref, ef_ref, inc_ref, gain_ref, w_ref,
    out_ref,
    w, inc, normed, sq, to_partner, from_partner, to_across, from_across, own,
    sq_out, sq_part, sq_cross, sq_far,
    w_sem, s_sem, r_sem,
):
    frame, row, core, hi = place()
    partner = row + 1 - 2 * core
    across = lax.rem(row + 2, 4)
    corner = lax.rem(partner + 2, 4)
    load = pltpu.make_async_copy(w_ref, w, w_sem)
    load.start()
    barrier = pltpu.get_barrier_semaphore()
    for peer in (partner, across):
        pl.semaphore_signal(barrier, inc=1, device_id=dev(frame, peer))
    for g in range(8):
        for r in range(4):
            for d in range(2):
                inc[d, r * 32 : r * 32 + 32, lanes(g)] = inc_ref[
                    g * 4 + r, d * 32 : d * 32 + 32
                ]

    order = (corner, across, partner, row)

    @pl.loop(0, 4)
    def _(n):
        target = jnp.where(
            n == 0, corner, jnp.where(n == 1, across, jnp.where(n == 2, partner, row))
        )
        rows = pl.ds(pl.multiple_of(target * BLK, BLK), BLK)
        ef = ef_ref[rows]
        total = jnp.zeros((BLK, 1), F32)
        for g in range(8):
            y = y_ref[rows, lanes(g)]
            for d in range(2):
                c = bc_ref[rows, d * 256 + 128 : d * 256 + 256]
                y = y + expand(ef, d * 16 + 2 * g) * dot(c, inc[d, :, lanes(g)])
            gated = y * silu(gate_ref[rows, lanes(g)].astype(F32))
            total = total + jnp.sum(gated * gated, axis=1, keepdims=True)
            normed[pl.ds(pl.multiple_of(n * BLK, BLK), BLK), lanes(g)] = (
                gated * gain_ref[:, lanes(g)]
            ).astype(BF)
        sq[n] = jnp.broadcast_to(total, (BLK, BLK)).T[0:8]

    load.wait()
    pl.semaphore_wait(barrier, 2)
    sq_out[0] = sq[0]
    sq_out[1] = sq[2]
    sq_copy = remote(sq_out, sq_part, s_sem.at[0], r_sem.at[0], dev(frame, partner))
    sq_copy.start()
    first, second, third = [], [], []
    for k in range(NCOL):
        cols = slice(k * COLS, (k + 1) * COLS)
        part = dot(normed[0:HALF, :], w[:, cols])
        to_partner[0, k] = part[0:BLK].astype(BF)
        copy = remote(
            to_partner.at[0, k], from_partner.at[0, k], s_sem.at[1 + k], r_sem.at[1 + k],
            dev(frame, partner),
        )
        copy.start()
        first.append(copy)
        own[k] = part[BLK:]

    sq_copy.wait_recv()
    sq_cross[...] = sq[1] + sq_part[0]
    far_copy = remote(sq_cross, sq_far, s_sem.at[1 + NCOL], r_sem.at[1 + NCOL], dev(frame, across))
    far_copy.start()
    for k in range(NCOL):
        first[k].wait_recv()
        to_across[k] = (own[k] + from_partner[0, k].astype(F32)).astype(BF)
        copy = remote(
            to_across.at[k], from_across.at[k], s_sem.at[2 + NCOL + k], r_sem.at[2 + NCOL + k],
            dev(frame, across),
        )
        copy.start()
        second.append(copy)
    for k in range(NCOL):
        cols = slice(k * COLS, (k + 1) * COLS)
        part = dot(normed[HALF:, :], w[:, cols])
        to_partner[1, k] = part[0:BLK].astype(BF)
        copy = remote(
            to_partner.at[1, k], from_partner.at[1, k],
            s_sem.at[2 + 2 * NCOL + k], r_sem.at[2 + 2 * NCOL + k],
            dev(frame, partner),
        )
        copy.start()
        third.append(copy)
        own[k] = part[BLK:]
    far_copy.wait_recv()
    mean = (sq[3] + sq_part[1] + sq_far[...]) * (1.0 / D_INNER)
    scale = jnp.broadcast_to(lax.rsqrt(mean + 1e-05)[0:1], (BLK, BLK)).T[:, 0:1]
    for k in range(NCOL):
        third[k].wait_recv()
        own[k] = own[k] + from_partner[1, k].astype(F32)
    for k in range(NCOL):
        cols = slice(k * COLS, (k + 1) * COLS)
        second[k].wait_recv()
        out_ref[:, cols] = (scale * (own[k] + from_across[k].astype(F32))).astype(BF)
    for copy in [sq_copy, far_copy] + first + second + third:
        copy.wait_send()


def finish(y, gate, bc, ef, inc, gain, w_out):
    return pl.pallas_call(
        finish_body,
        name="finish",
        out_shape=jax.ShapeDtypeStruct((BLK, D), BF),
        in_specs=[VM] * 6 + [ANY],
        out_specs=VM,
        scratch_shapes=[
            pltpu.VMEM((CH, D), BF),
            pltpu.VMEM((2, 128, CH), BF),
            pltpu.VMEM((TOK, CH), BF),
            pltpu.VMEM((4, 8, 128), F32),
            pltpu.VMEM((2, NCOL, BLK, COLS), BF),
            pltpu.VMEM((2, NCOL, BLK, COLS), BF),
            pltpu.VMEM((NCOL, BLK, COLS), BF),
            pltpu.VMEM((NCOL, BLK, COLS), BF),
            pltpu.VMEM((NCOL, BLK, COLS), F32),
            pltpu.VMEM((2, 8, 128), F32),
            pltpu.VMEM((2, 8, 128), F32),
            pltpu.VMEM((8, 128), F32),
            pltpu.VMEM((8, 128), F32),
            pltpu.SemaphoreType.DMA,
            pltpu.SemaphoreType.DMA((2 + 3 * NCOL,)),
            pltpu.SemaphoreType.DMA((2 + 3 * NCOL,)),
        ],
        compiler_params=pltpu.CompilerParams(
            collective_id=2, has_side_effects=True, vmem_limit_bytes=60 * 1024 * 1024
        ),
    )(y, gate, bc, ef, inc, gain, w_out)


def per_device(
    tokens, w_gate, w_value, w_state_proj, w_step, step_bias, decay_rate, conv_taps,
    skip_gain, norm_gain, w_out,
):
    params = jnp.stack([step_bias.reshape(32), decay_rate.reshape(32), skip_gain.reshape(32)])
    params = jnp.pad(params, ((0, 5), (0, 96)))
    gate, x_raw, halo, bc, step = project(tokens[0], w_gate, w_value, w_state_proj, w_step)
    msg, y, ef = local_scan(x_raw, halo, bc, step, params, conv_taps)
    inc = exchange(msg)
    out = finish(y, gate, bc, ef, inc, norm_gain[None, :], w_out)
    return out[None]


def solution(mesh):
    in_specs = (
        P("frame", "row", None), P(None, "row"), P(None, "row"), P(), P(None, None, "row"),
        P(None, "row"), P(None, "row"), P(None, None, "row"), P(None, "row"), P("row"),
        P("row", None),
    )
    return jax.shard_map(
        per_device, mesh=mesh, in_specs=in_specs, out_specs=P("frame", "row", None),
        check_vma=False,
    )
```

```python
import jax
import jax.numpy as jnp
from jax import lax
from jax.experimental import pallas as pl
from jax.experimental.pallas import tpu as pltpu
from jax.sharding import PartitionSpec as P

BF = jnp.bfloat16
F32 = jnp.float32
FRAMES = 32
TOK = 512
BLK = 128
NBLK = 4
CH = 1024
D = 2048
HALF = 256
HALO = 8
LOG2E = 1.4426950408889634
D_INNER = 4096
VM = pl.BlockSpec(memory_space=pltpu.VMEM)
ANY = pl.BlockSpec(memory_space=pl.ANY)
MSG = 72


def silu(x):
    return 0.5 * x * (1.0 + jnp.tanh(0.5 * x))


def dot(a, b):
    return jnp.dot(a, b, preferred_element_type=F32)


def dev(frame, row):
    return {"frame": frame, "row": row}


def place():
    frame, row = lax.axis_index("frame"), lax.axis_index("row")
    core = lax.rem(row, 2)
    return frame, row, core, lax.div(row, 2)


def remote(src, dst, send, recv, target):
    return pltpu.make_async_remote_copy(src, dst, send, recv, device_id=target)


CHUNKS = 4
CROWS = 128 // CHUNKS
EDGE = 16
COLS = 512
NCOL = D // COLS
PEERS = FRAMES - 1


def expand(values, base):
    lane = lax.broadcasted_iota(jnp.int32, (1, 128), 1)
    return jnp.where(lane < 64, values[:, base : base + 1], values[:, base + 1 : base + 2])


def lanes(group):
    return slice(group * 128, group * 128 + 128)


def block(j, count=BLK, shift=0):
    return pl.ds(pl.multiple_of(j * BLK + shift, 16), count)


def layer_body(
    tok_ref, wg_ref, wv_ref, ws_ref, wt_ref, wo_ref,
    bias_ref, rate_ref, skip_ref, taps_ref, gain_ref,
    out_ref,
    tb, edge, wg, wv, ws, wt, wo, par, gate, bc,
    xp, xs, xdt, start, upd, car, cum_s, dt_s, tot_s, y_s, ef_s,
    msg, got, ret, inc, inc_m,
    normed, sq, to_partner, from_partner, to_across, from_across, own,
    sq_out, sq_part, sq_cross, sq_far,
    w_sem, g_s, g_r, a_s, a_r, b_s, b_r, f_s, f_r,
):
    frame, row, core, hi = place()
    partner = row + 1 - 2 * core
    across = lax.rem(row + 2, 4)
    corner = lax.rem(partner + 2, 4)
    peers = [lax.rem(frame + i, FRAMES) for i in range(1, FRAMES)]
    first, final = frame == 0, frame == FRAMES - 1

    mine = pl.ds(pl.multiple_of(EDGE + row * BLK, 16), BLK)
    loads = []
    for i, (src, dst) in enumerate((
        (tok_ref, tb.at[mine]), (wv_ref, wv), (ws_ref, ws),
        (wt_ref.at[0], wt.at[0:16]), (wt_ref.at[1], wt.at[16:32]),
        (wg_ref, wg), (wo_ref, wo),
    )):
        copy = pltpu.make_async_copy(src, dst, w_sem.at[i])
        copy.start()
        loads.append(copy)
    tb[0:EDGE, :] = jnp.zeros((EDGE, D), BF)
    tb[EDGE + TOK :, :] = jnp.zeros((EDGE, D), BF)
    barrier = pltpu.get_barrier_semaphore()
    for peer in (partner, across):
        pl.semaphore_signal(barrier, inc=1, device_id=dev(frame, peer))
    for peer in peers:
        pl.semaphore_signal(barrier, inc=1, device_id=dev(peer, row))

    @pl.when(jnp.logical_not(first))
    def _():
        pl.semaphore_signal(barrier, inc=1, device_id=dev(frame - 1, 3))

    @pl.when(jnp.logical_not(final))
    def _():
        pl.semaphore_signal(barrier, inc=1, device_id=dev(frame + 1, 0))

    to_next = jnp.logical_and(row == 3, jnp.logical_not(final))
    to_prev = jnp.logical_and(row == 0, jnp.logical_not(first))
    wt[32:128, :] = jnp.zeros((96, D), BF)
    par[...] = jnp.zeros_like(par)
    for i, ref in enumerate((bias_ref, rate_ref, skip_ref)):
        for d in range(2):
            par[i : i + 1, d * 16 : d * 16 + 16] = ref[d : d + 1, :]
    loads[0].wait()
    pl.semaphore_wait(
        barrier, 2 + PEERS + jnp.where(jnp.logical_or(to_next, to_prev), 4, 0)
    )

    def chunk_rows(owner, i, sender_hi):
        at = jnp.where(sender_hi == 1, i, CHUNKS - 1 - i) * CROWS
        return pl.ds(pl.multiple_of(EDGE + owner * BLK + at, 16), CROWS)

    def cross(i, owner, sender_hi):
        rows = chunk_rows(owner, i, sender_hi)
        return remote(tb.at[rows], tb.at[rows], g_s.at[i], g_r.at[i], dev(frame, across))

    def forward(i):
        rows = chunk_rows(across, i, 1 - hi)
        return remote(
            tb.at[rows], tb.at[rows], g_s.at[CHUNKS + i], g_r.at[CHUNKS + i], dev(frame, partner)
        )

    def forwarded(i):
        rows = chunk_rows(corner, i, 1 - hi)
        return remote(
            tb.at[rows], tb.at[rows], g_s.at[CHUNKS + i], g_r.at[CHUNKS + i], dev(frame, partner)
        )

    def pass_on(i):
        cross(i, across, 1 - hi).wait_recv()
        forward(i).start()

    near = remote(
        tb.at[mine], tb.at[mine], g_s.at[2 * CHUNKS], g_r.at[2 * CHUNKS], dev(frame, partner)
    )

    def halo_copies(up):
        src = tb.at[pl.ds(pl.multiple_of(EDGE + row * BLK + (BLK - HALO if up else 0), HALO), HALO)]
        dst = tb.at[pl.ds(EDGE - HALO if up else EDGE + TOK, HALO)]
        base = 2 * CHUNKS + 1 + (0 if up else 4)
        return [
            remote(
                src, dst, g_s.at[base + r], g_r.at[2 * CHUNKS + 1 + (0 if up else 1)],
                dev(frame + 1 if up else frame - 1, r),
            )
            for r in range(4)
        ]

    near.start()
    cross(0, row, hi).start()
    for up, flag in ((True, to_next), (False, to_prev)):

        @pl.when(flag)
        def _(up=up):
            for copy in halo_copies(up):
                copy.start()

    for i in range(1, CHUNKS):
        cross(i, row, hi).start()

    def over(read, weight, columns, width, store):
        @pl.loop(0, columns // width)
        def _(n):
            cols = pl.ds(pl.multiple_of(n * width, width), width)
            store(dot(read(), weight[:, cols]), cols)

    def phase(half, waits):
        def read():
            return tb[pl.ds(pl.multiple_of(EDGE + half * HALF, 16), HALF), :]

        rows = pl.ds(pl.multiple_of(half * HALF, 16), HALF)
        rows_x = pl.ds(pl.multiple_of(EDGE + half * HALF, 16), HALF)

        def put_x(out, cols):
            xp[rows_x, cols] = out.astype(BF).astype(F32)

        def put_bc(out, cols):
            bc[rows, cols] = out.astype(BF)

        if waits:
            loads[1].wait()
        over(read, wv, CH, 256, put_x)
        if waits:
            loads[2].wait()
        over(read, ws, 512, 256, put_bc)
        if waits:
            loads[3].wait()
            loads[4].wait()
        raw = lax.dot_general(
            read(), wt[...], (((1,), (1,)), ((), ())), preferred_element_type=F32
        ).astype(BF).astype(F32) + par[0:1, :]
        dt_s[rows, :] = jnp.maximum(raw, 0.0) + jnp.log1p(jnp.exp(-jnp.abs(raw)))

    row_i = lax.broadcasted_iota(jnp.int32, (BLK, BLK), 0)
    col_i = lax.broadcasted_iota(jnp.int32, (BLK, BLK), 1)
    lower, upper = row_i >= col_i, col_i >= row_i
    fwd_lane = col_i < 16

    def prepare(j):
        rows = block(j)
        part = dt_s[rows, :] * (par[1:2, :] * -LOG2E)
        high = part.astype(BF)
        rest = part - high.astype(F32)
        mid = rest.astype(BF)
        low = (rest - mid.astype(F32)).astype(BF)
        tri = lower.astype(BF)
        cum = dot(tri, high) + (dot(tri, mid) + dot(tri, low))
        total = cum[BLK - 1 : BLK]
        cum_s[rows, :] = jnp.where(fwd_lane, cum, (total - cum) + part)
        tot_s[pl.ds(j, 1), :] = total

    def convolve(j):
        for g in range(8):
            window = xp[block(j, BLK + 2 * EDGE), lanes(g)]
            size = BLK + 2 * EDGE
            shifted = {
                o: pltpu.roll(window, (-o) % size, 0)[EDGE : EDGE + BLK] if o
                else window[EDGE : EDGE + BLK]
                for o in range(-3, 4)
            }
            for d in range(2):
                acc = None
                for k in range(4):
                    term = taps_ref[d, k : k + 1, lanes(g)] * shifted[3 - k if d else k - 3]
                    acc = term if acc is None else acc + term
                xs[d, block(j), lanes(g)] = silu(acc).astype(BF)

    def update(j):
        rows = block(j)
        total = tot_s[pl.ds(j, 1), :]
        dt_j = dt_s[rows, :]
        fade = jnp.exp2(total - cum_s[rows, :]) * dt_j
        for d in range(2):
            b = bc[rows, d * 256 : d * 256 + 128]
            bt = b.astype(F32).T.astype(BF)
            for g in range(8):
                x = xs[d, rows, lanes(g)].astype(F32)
                xdt[d, rows, lanes(g)] = (x * expand(dt_j, d * 16 + 2 * g)).astype(BF)
                carried = (x * expand(fade, d * 16 + 2 * g)).astype(BF)
                upd[d, pl.ds(j, 1), :, lanes(g)] = dot(bt, carried)[None]

    def intra(j):
        rows = block(j)
        cum = cum_s[rows, :]
        cum_t = cum.T
        skip = par[2:3, :]
        scores = []
        for d in range(2):
            s = lax.dot_general(
                bc[rows, d * 256 + 128 : d * 256 + 256], bc[rows, d * 256 : d * 256 + 128],
                (((1,), (1,)), ((), ())), preferred_element_type=F32,
            )
            scores.append(jnp.where(lower if d == 0 else upper, s, 0.0))
        for g in range(8):
            values = jnp.concatenate([xdt[0, rows, lanes(g)], xdt[1, rows, lanes(g)]], axis=0)
            outs = []
            for k in range(2):
                w = []
                for d in range(2):
                    n = d * 16 + 2 * g + k
                    gap = jnp.minimum(cum[:, n : n + 1] - cum_t[n : n + 1, :], 0.0)
                    w.append((scores[d] * jnp.exp2(gap)).astype(BF))
                outs.append(dot(jnp.concatenate(w, axis=1), values))
            y = jnp.where(col_i < 64, outs[0], outs[1])
            for d in range(2):
                y = y + expand(skip, d * 16 + 2 * g) * xs[d, rows, lanes(g)].astype(F32)
            y_s[rows, lanes(g)] = y

    near.wait_recv()
    phase(hi, True)
    pass_on(0)
    for up, flag in ((True, first), (False, final)):

        @pl.when(jnp.logical_not(flag))
        def _(up=up):
            halo_copies(up)[0].wait_recv()

    forwarded(0).wait_recv()
    beside = pl.ds(pl.multiple_of(jnp.where(hi == 0, EDGE + HALF, HALF), 16), EDGE)
    edge[0:16, :] = tb[0:EDGE, :]
    edge[16:32, :] = tb[beside, :]
    edge[32:48, :] = tb[EDGE + TOK :, :]

    def put_edge(out, cols):
        out = out.astype(BF).astype(F32)
        xp[0:EDGE, cols] = out[0:16]
        xp[beside, cols] = out[16:32]
        xp[EDGE + TOK :, cols] = out[32:48]

    over(lambda: edge[...], wv, CH, 256, put_edge)

    @pl.loop(0, 2)
    def _(i):
        j = hi * 2 + i
        prepare(j)
        convolve(j)
        update(j)
        pass_on(1 + i)

    @pl.loop(0, 2)
    def _(i):
        intra(hi * 2 + i)

        @pl.when(i == 0)
        def _():
            pass_on(3)

    for i in range(1, CHUNKS):
        forwarded(i).wait_recv()
    phase(1 - hi, False)

    @pl.loop(0, 2)
    def _(i):
        j = (1 - hi) * 2 + i
        prepare(j)
        convolve(j)
        update(j)

    row8 = lax.broadcasted_iota(jnp.int32, (8, 128), 0)
    shrink = jnp.exp2(tot_s[...])
    whole = jnp.exp2(tot_s[0:1, :] + tot_s[1:2, :] + tot_s[2:3, :] + tot_s[3:4, :])
    for g in range(8):
        tail = jnp.zeros((8, 128), F32)
        for d in range(2):
            base = d * 16 + 2 * g
            decay = expand(whole, base)
            high = decay.astype(BF).astype(F32)
            tail = jnp.where(row8 == 2 * d, high, tail)
            tail = jnp.where(row8 == 2 * d + 1, decay - high, tail)
            order = range(NBLK) if d == 0 else range(NBLK - 1, -1, -1)
            state = None
            for j in order:
                new = upd[d, j, :, lanes(g)]
                if state is None:
                    state = new
                else:
                    start[d, j, :, lanes(g)] = state.astype(BF)
                    state = state * expand(shrink[j : j + 1], base) + new
            state = state.astype(BF)
            for r in range(4):
                msg[g * 4 + r, d * 32 : d * 32 + 32] = state[r * 32 : r * 32 + 32]
        for r in range(4):
            msg[g * 4 + r, 64:72] = tail.astype(BF)

    def everywhere(src, dst, send, recv):
        copies = []
        for i, peer in enumerate(peers):
            copy = remote(src.at[peer], dst.at[frame], send.at[i], recv.at[i], dev(peer, row))
            copy.start()
            copies.append(copy)
        dst[frame] = src[frame]
        return copies

    there = everywhere(msg, got, a_s, a_r)

    @pl.loop(0, 2)
    def _(i):
        intra((1 - hi) * 2 + i)

    for copy in there:
        copy.wait_recv()
    for d in range(2):
        state = jnp.zeros((32, 128), F32)
        for g in range(FRAMES) if d == 0 else reversed(range(FRAMES)):
            ret[g, d * 32 : d * 32 + 32] = state.astype(BF)
            tail = got[g, 64:72].astype(F32)
            decay = tail[2 * d : 2 * d + 1] + tail[2 * d + 1 : 2 * d + 2]
            state = decay * state + got[g, d * 32 : d * 32 + 32].astype(F32)
    back = everywhere(ret, inc, b_s, b_r)

    loads[5].wait()

    def put_gate(out, cols):
        gate[:, cols] = out.astype(BF)

    over(lambda: tb[EDGE : EDGE + TOK, :], wg, CH, 256, put_gate)

    def from_start(j, d):
        rows = block(j)
        grown = jnp.exp2(cum_s[rows, :])
        c = bc[rows, d * 256 + 128 : d * 256 + 256]
        for g in range(8):
            y_s[rows, lanes(g)] += expand(grown, d * 16 + 2 * g) * dot(c, start[d, j, :, lanes(g)])

    @pl.loop(0, NBLK - 1)
    def _(i):
        from_start(i + 1, 0)
        from_start(i, 1)

    zero = jnp.zeros((1, 128), F32)
    before, after = [zero], [zero]
    for j in range(NBLK - 1):
        before.append(before[-1] + tot_s[j : j + 1, :])
        after.append(after[-1] + tot_s[NBLK - 1 - j : NBLK - j, :])
    after = after[::-1]
    for j in range(NBLK):
        rows = slice(j * BLK, (j + 1) * BLK)
        ef_s[rows, :] = jnp.exp2(cum_s[rows, :] + jnp.where(fwd_lane[0:1], before[j], after[j]))
    for copy in back:
        copy.wait_recv()
    for g in range(8):
        for r in range(4):
            for d in range(2):
                inc_m[d, r * 32 : r * 32 + 32, lanes(g)] = inc[g * 4 + r, d * 32 : d * 32 + 32]

    def gated_rows(n, target):
        rows = block(target)
        ef = ef_s[rows, :]
        total = jnp.zeros((BLK, 1), F32)
        for g in range(8):
            y = y_s[rows, lanes(g)]
            for d in range(2):
                c = bc[rows, d * 256 + 128 : d * 256 + 256]
                y = y + expand(ef, d * 16 + 2 * g) * dot(c, inc_m[d, :, lanes(g)])
            gated = y * silu(gate[rows, lanes(g)].astype(F32))
            total = total + jnp.sum(gated * gated, axis=1, keepdims=True)
            normed[block(n), lanes(g)] = (gated * gain_ref[:, lanes(g)]).astype(BF)
        sq[n] = jnp.broadcast_to(total, (BLK, BLK)).T[0:8]

    @pl.loop(0, 2)
    def _(n):
        gated_rows(n, jnp.where(n == 0, corner, across))

    loads[6].wait()
    ones, twos, threes = [], [], []
    for k in range(NCOL):
        cols = slice(k * COLS, (k + 1) * COLS)
        part = dot(normed[0:HALF, :], wo[:, cols])
        to_partner[0, k] = part[0:BLK].astype(BF)
        copy = remote(
            to_partner.at[0, k], from_partner.at[0, k], f_s.at[k], f_r.at[k], dev(frame, partner)
        )
        copy.start()
        ones.append(copy)
        own[k] = part[BLK:]
    for k in range(NCOL):
        ones[k].wait_recv()
        to_across[k] = (own[k] + from_partner[0, k].astype(F32)).astype(BF)
        copy = remote(
            to_across.at[k], from_across.at[k], f_s.at[NCOL + k], f_r.at[NCOL + k],
            dev(frame, across),
        )
        copy.start()
        twos.append(copy)

    @pl.loop(2, 4)
    def _(n):
        gated_rows(n, jnp.where(n == 2, partner, row))

    sq_out[0] = sq[0]
    sq_out[1] = sq[2]
    sq_copy = remote(sq_out, sq_part, f_s.at[3 * NCOL], f_r.at[3 * NCOL], dev(frame, partner))
    sq_copy.start()
    for k in range(NCOL):
        cols = slice(k * COLS, (k + 1) * COLS)
        part = dot(normed[HALF:, :], wo[:, cols])
        to_partner[1, k] = part[0:BLK].astype(BF)
        copy = remote(
            to_partner.at[1, k], from_partner.at[1, k], f_s.at[2 * NCOL + k],
            f_r.at[2 * NCOL + k], dev(frame, partner),
        )
        copy.start()
        threes.append(copy)
        own[k] = part[BLK:]
    sq_copy.wait_recv()
    sq_cross[...] = sq[1] + sq_part[0]
    far_copy = remote(
        sq_cross, sq_far, f_s.at[3 * NCOL + 1], f_r.at[3 * NCOL + 1], dev(frame, across)
    )
    far_copy.start()
    for k in range(NCOL):
        threes[k].wait_recv()
        own[k] = own[k] + from_partner[1, k].astype(F32)
    far_copy.wait_recv()
    mean = (sq[3] + sq_part[1] + sq_far[...]) * (1.0 / D_INNER)
    scale = jnp.broadcast_to(lax.rsqrt(mean + 1e-05)[0:1], (BLK, BLK)).T[:, 0:1]
    for k in range(NCOL):
        cols = slice(k * COLS, (k + 1) * COLS)
        twos[k].wait_recv()
        out_ref[:, cols] = (scale * (own[k] + from_across[k].astype(F32))).astype(BF)

    near.wait_send()
    for i in range(CHUNKS):
        cross(i, row, hi).wait_send()
        forward(i).wait_send()
    for up, flag in ((True, to_next), (False, to_prev)):

        @pl.when(flag)
        def _(up=up):
            for copy in halo_copies(up):
                copy.wait_send()

    for copy in there + back + ones + twos + threes + [sq_copy, far_copy]:
        copy.wait_send()


def layer(*operands):
    dma = pltpu.SemaphoreType.DMA
    vmem = pltpu.VMEM
    return pl.pallas_call(
        layer_body,
        name="layer",
        out_shape=jax.ShapeDtypeStruct((BLK, D), BF),
        in_specs=[ANY] * 6 + [VM] * 5,
        out_specs=VM,
        scratch_shapes=[
            vmem((TOK + 2 * EDGE, D), BF), vmem((48, D), BF),
            vmem((D, CH), BF), vmem((D, CH), BF), vmem((D, 512), BF), vmem((128, D), BF),
            vmem((CH, D), BF), vmem((8, 128), F32), vmem((TOK, CH), BF), vmem((TOK, 512), BF),
            vmem((TOK + 2 * EDGE, CH), F32),
            vmem((2, TOK, CH), BF), vmem((2, TOK, CH), BF),
            vmem((2, NBLK, 128, CH), BF), vmem((2, NBLK, 128, CH), F32), vmem((BLK, CH), BF),
            vmem((TOK, 128), F32), vmem((TOK, 128), F32), vmem((8, 128), F32),
            vmem((TOK, CH), F32), vmem((TOK, 128), F32),
            vmem((FRAMES, MSG, 128), BF), vmem((FRAMES, MSG, 128), BF),
            vmem((FRAMES, 64, 128), BF), vmem((FRAMES, 64, 128), BF), vmem((2, 128, CH), BF),
            vmem((TOK, CH), BF), vmem((4, 8, 128), F32),
            vmem((2, NCOL, BLK, COLS), BF), vmem((2, NCOL, BLK, COLS), BF),
            vmem((NCOL, BLK, COLS), BF), vmem((NCOL, BLK, COLS), BF),
            vmem((NCOL, BLK, COLS), F32),
            vmem((2, 8, 128), F32), vmem((2, 8, 128), F32), vmem((8, 128), F32),
            vmem((8, 128), F32),
            dma((7,)), dma((2 * CHUNKS + 9,)), dma((2 * CHUNKS + 3,)),
            dma((PEERS,)), dma((PEERS,)), dma((PEERS,)), dma((PEERS,)),
            dma((3 * NCOL + 2,)), dma((3 * NCOL + 2,)),
        ],
        compiler_params=pltpu.CompilerParams(
            collective_id=0, has_side_effects=True, vmem_limit_bytes=62 * 1024 * 1024
        ),
    )(*operands)


def per_device(
    tokens, w_gate, w_value, w_state_proj, w_step, step_bias, decay_rate, conv_taps,
    skip_gain, norm_gain, w_out,
):
    out = layer(
        tokens[0], w_gate, w_value, w_state_proj, jnp.swapaxes(w_step, 1, 2), w_out,
        step_bias, decay_rate, skip_gain, conv_taps, norm_gain[None, :],
    )
    return out[None]


def solution(mesh):
    in_specs = (
        P("frame", "row", None), P(None, "row"), P(None, "row"), P(), P(None, None, "row"),
        P(None, "row"), P(None, "row"), P(None, None, "row"), P(None, "row"), P("row"),
        P("row", None),
    )
    return jax.shard_map(
        per_device, mesh=mesh, in_specs=in_specs, out_specs=P("frame", "row", None),
        check_vma=False,
    )
```

```python
import jax
import jax.numpy as jnp
from jax import lax
from jax.experimental import pallas as pl
from jax.experimental.pallas import tpu as pltpu
from jax.sharding import PartitionSpec as P

BF = jnp.bfloat16
F32 = jnp.float32
FRAMES = 32
TOK = 512
BLK = 128
NBLK = 4
CH = 1024
D = 2048
HALF = 256
HALO = 8
LOG2E = 1.4426950408889634
D_INNER = 4096
VM = pl.BlockSpec(memory_space=pltpu.VMEM)
ANY = pl.BlockSpec(memory_space=pl.ANY)
MSG = 72


def silu(x):
    return 0.5 * x * (1.0 + jnp.tanh(0.5 * x))


def dot(a, b):
    return jnp.dot(a, b, preferred_element_type=F32)


def dev(frame, row):
    return {"frame": frame, "row": row}


def place():
    frame, row = lax.axis_index("frame"), lax.axis_index("row")
    core = lax.rem(row, 2)
    return frame, row, core, lax.div(row, 2)


def remote(src, dst, send, recv, target):
    return pltpu.make_async_remote_copy(src, dst, send, recv, device_id=target)


CHUNKS = 4
CROWS = 128 // CHUNKS
EDGE = 16
COLS = 512
LAG = 2
NCOL = D // COLS
PEERS = FRAMES - 1
STEPS = sorted(
    ((dx, dy, dz) for dx in range(4) for dy in range(4) for dz in range(2) if dx + dy + dz),
    key=lambda s: -(min(s[0], 4 - s[0]) + min(s[1], 4 - s[1]) + s[2]),
)


def expand(values, base):
    lane = lax.broadcasted_iota(jnp.int32, (1, 128), 1)
    return jnp.where(lane < 64, values[:, base : base + 1], values[:, base + 1 : base + 2])


def lanes(group):
    return slice(group * 128, group * 128 + 128)


def block(j, count=BLK, shift=0):
    return pl.ds(pl.multiple_of(j * BLK + shift, 16), count)


def layer_body(
    tok_ref, wg_ref, wv_ref, ws_ref, wt_ref, wo_ref,
    bias_ref, rate_ref, skip_ref, taps_ref, gain_ref,
    out_ref,
    tb, edge, wg, wv, ws, wt, wo, par, gate, bc,
    xp, xs, start, upd, car, cum_s, dt_s, tot_s, y_s, ef_s, off_s,
    msg, got, ret, inc, inc_m,
    normed, sq, to_partner, from_partner, to_across, from_across, own,
    sq_out, sq_part, sq_cross, sq_far,
    w_sem, g_s, g_r, a_s, a_r, b_s, b_r, f_s, f_r,
):
    frame, row, core, hi = place()
    partner = row + 1 - 2 * core
    across = lax.rem(row + 2, 4)
    corner = lax.rem(partner + 2, 4)
    fx, fy, fz = lax.div(frame, 8), lax.rem(lax.div(frame, 2), 4), lax.rem(frame, 2)
    peers = [
        lax.rem(fx + dx, 4) * 8 + lax.rem(fy + dy, 4) * 2 + lax.rem(fz + dz, 2)
        for dx, dy, dz in STEPS
    ]
    first, final = frame == 0, frame == FRAMES - 1

    mine = pl.ds(pl.multiple_of(EDGE + row * BLK, 16), BLK)
    loads = []
    for i, (src, dst) in enumerate((
        (tok_ref, tb.at[mine]), (wv_ref, wv), (ws_ref, ws),
        (wt_ref.at[0], wt.at[0:16]), (wt_ref.at[1], wt.at[16:32]),
        (wg_ref, wg), (wo_ref, wo),
    )):
        copy = pltpu.make_async_copy(src, dst, w_sem.at[i])
        copy.start()
        loads.append(copy)
    tb[0:EDGE, :] = jnp.zeros((EDGE, D), BF)
    tb[EDGE + TOK :, :] = jnp.zeros((EDGE, D), BF)
    barrier = pltpu.get_barrier_semaphore()
    for peer in (partner, across):
        pl.semaphore_signal(barrier, inc=1, device_id=dev(frame, peer))
    for peer in peers:
        pl.semaphore_signal(barrier, inc=1, device_id=dev(peer, row))

    @pl.when(jnp.logical_not(first))
    def _():
        pl.semaphore_signal(barrier, inc=1, device_id=dev(frame - 1, 3))

    @pl.when(jnp.logical_not(final))
    def _():
        pl.semaphore_signal(barrier, inc=1, device_id=dev(frame + 1, 0))

    to_next = jnp.logical_and(row == 3, jnp.logical_not(final))
    to_prev = jnp.logical_and(row == 0, jnp.logical_not(first))
    wt[32:128, :] = jnp.zeros((96, D), BF)
    par[...] = jnp.zeros_like(par)
    for i, ref in enumerate((bias_ref, rate_ref, skip_ref)):
        for d in range(2):
            par[i : i + 1, d * 16 : d * 16 + 16] = ref[d : d + 1, :]
    loads[0].wait()
    pl.semaphore_wait(
        barrier, 2 + PEERS + jnp.where(jnp.logical_or(to_next, to_prev), 4, 0)
    )

    def chunk_rows(owner, i, sender_hi):
        at = jnp.where(sender_hi == 1, i, CHUNKS - 1 - i) * CROWS
        return pl.ds(pl.multiple_of(EDGE + owner * BLK + at, 16), CROWS)

    def cross(i, owner, sender_hi):
        rows = chunk_rows(owner, i, sender_hi)
        return remote(tb.at[rows], tb.at[rows], g_s.at[i], g_r.at[i], dev(frame, across))

    def forward(i):
        rows = chunk_rows(across, i, 1 - hi)
        return remote(
            tb.at[rows], tb.at[rows], g_s.at[CHUNKS + i], g_r.at[CHUNKS + i], dev(frame, partner)
        )

    def forwarded(i):
        rows = chunk_rows(corner, i, 1 - hi)
        return remote(
            tb.at[rows], tb.at[rows], g_s.at[CHUNKS + i], g_r.at[CHUNKS + i], dev(frame, partner)
        )

    def pass_on(i):
        cross(i, across, 1 - hi).wait_recv()
        forward(i).start()

    near = remote(
        tb.at[mine], tb.at[mine], g_s.at[2 * CHUNKS], g_r.at[2 * CHUNKS], dev(frame, partner)
    )

    def halo_copies(up):
        src = tb.at[pl.ds(pl.multiple_of(EDGE + row * BLK + (BLK - HALO if up else 0), HALO), HALO)]
        dst = tb.at[pl.ds(EDGE - HALO if up else EDGE + TOK, HALO)]
        base = 2 * CHUNKS + 1 + (0 if up else 4)
        return [
            remote(
                src, dst, g_s.at[base + r], g_r.at[2 * CHUNKS + 1 + (0 if up else 1)],
                dev(frame + 1 if up else frame - 1, r),
            )
            for r in range(4)
        ]

    near.start()
    cross(0, row, hi).start()
    for up, flag in ((True, to_next), (False, to_prev)):

        @pl.when(flag)
        def _(up=up):
            for copy in halo_copies(up):
                copy.start()

    for i in range(1, CHUNKS):
        cross(i, row, hi).start()

    def over(read, weight, columns, width, store):
        @pl.loop(0, columns // width)
        def _(n):
            cols = pl.ds(pl.multiple_of(n * width, width), width)
            store(dot(read(), weight[:, cols]), cols)

    def phase(half, waits):
        def read():
            return tb[pl.ds(pl.multiple_of(EDGE + half * HALF, 16), HALF), :]

        rows = pl.ds(pl.multiple_of(half * HALF, 16), HALF)
        rows_x = pl.ds(pl.multiple_of(EDGE + half * HALF, 16), HALF)

        def read_x():
            return read() if waits else jnp.concatenate([read(), edge[...]], axis=0)

        def put_x(out, cols):
            out = out.astype(BF).astype(F32)
            xp[rows_x, cols] = out[:HALF]
            if not waits:
                xp[0:EDGE, cols] = out[HALF : HALF + EDGE]
                xp[EDGE + TOK :, cols] = out[HALF + EDGE :]

        def put_bc(out, cols):
            bc[rows, cols] = out.astype(BF)

        if waits:
            loads[1].wait()
        over(read_x, wv, CH, 512, put_x)
        if waits:
            loads[2].wait()
        over(read, ws, 512, 512, put_bc)
        if waits:
            loads[3].wait()
            loads[4].wait()
        raw = lax.dot_general(
            read(), wt[...], (((1,), (1,)), ((), ())), preferred_element_type=F32
        ).astype(BF).astype(F32) + par[0:1, :]
        dt_s[rows, :] = jnp.maximum(raw, 0.0) + jnp.log1p(jnp.exp(-jnp.abs(raw)))

    row_i = lax.broadcasted_iota(jnp.int32, (BLK, BLK), 0)
    col_i = lax.broadcasted_iota(jnp.int32, (BLK, BLK), 1)
    lower, upper = row_i >= col_i, col_i >= row_i
    fwd_lane = col_i < 16

    def prepare(j):
        rows = block(j)
        part = dt_s[rows, :] * (par[1:2, :] * -LOG2E)
        high = part.astype(BF)
        rest = part - high.astype(F32)
        mid = rest.astype(BF)
        low = (rest - mid.astype(F32)).astype(BF)
        tri = lower.astype(BF)
        cum = dot(tri, high) + (dot(tri, mid) + dot(tri, low))
        total = cum[BLK - 1 : BLK]
        cum_s[rows, :] = jnp.where(fwd_lane, cum, (total - cum) + part)
        tot_s[pl.ds(j, 1), :] = total

    def scan_in(j, d):
        size = BLK + 2 * EDGE
        rows = block(j)
        fade = jnp.exp2(tot_s[pl.ds(j, 1), :] - cum_s[rows, :]) * dt_s[rows, :]
        bt = bc[rows, d * 256 : d * 256 + 128].astype(F32).T.astype(BF)
        for g in range(8):
            window = xp[block(j, size), lanes(g)]
            acc = None
            for k in range(4):
                o = 3 - k if d else k - 3
                moved = pltpu.roll(window, (-o) % size, 0) if o else window
                term = taps_ref[d, k : k + 1, lanes(g)] * moved[EDGE : EDGE + BLK]
                acc = term if acc is None else acc + term
            x = silu(acc).astype(BF)
            xs[d, rows, lanes(g)] = x
            carried = (x.astype(F32) * expand(fade, d * 16 + 2 * g)).astype(BF)
            upd[d, pl.ds(j, 1), :, lanes(g)] = dot(bt, carried)[None]

    def intra(j):
        rows = block(j)
        cum = cum_s[rows, :]
        cum_t, dt_t = cum.T, dt_s[rows, :].T
        skip = par[2:3, :]
        scores = []
        for d in range(2):
            s = lax.dot_general(
                bc[rows, d * 256 + 128 : d * 256 + 256], bc[rows, d * 256 : d * 256 + 128],
                (((1,), (1,)), ((), ())), preferred_element_type=F32,
            )
            scores.append(jnp.where(lower if d == 0 else upper, s, 0.0))
        for g in range(8):
            values = jnp.concatenate([xs[0, rows, lanes(g)], xs[1, rows, lanes(g)]], axis=0)
            outs = []
            for k in range(2):
                w = []
                for d in range(2):
                    n = d * 16 + 2 * g + k
                    gap = jnp.minimum(cum[:, n : n + 1] - cum_t[n : n + 1, :], 0.0)
                    w.append((scores[d] * jnp.exp2(gap) * dt_t[n : n + 1, :]).astype(BF))
                outs.append(dot(jnp.concatenate(w, axis=1), values))
            y = jnp.where(col_i < 64, outs[0], outs[1])
            for d in range(2):
                y = y + expand(skip, d * 16 + 2 * g) * xs[d, rows, lanes(g)].astype(F32)
            y_s[rows, lanes(g)] = y

    near.wait_recv()
    phase(hi, True)
    pass_on(0)
    forwarded(0).wait_recv()
    beside = pl.ds(pl.multiple_of(jnp.where(hi == 0, EDGE + HALF, HALF), 16), EDGE)

    def put_edge(out, cols):
        xp[beside, cols] = out.astype(BF).astype(F32)

    over(lambda: tb[beside, :], wv, CH, 512, put_edge)

    prepare(hi * 2)
    prepare(hi * 2 + 1)
    for d in range(2):
        scan_in(1 + hi, d)
        pass_on(1 + d)
    for h in range(2):

        @pl.when(hi == h)
        def _(h=h):
            scan_in(3 * h, 1 - h)

    pass_on(3)
    for i in range(1, CHUNKS):
        forwarded(i).wait_recv()
    for up, flag in ((True, first), (False, final)):

        @pl.when(jnp.logical_not(flag))
        def _(up=up):
            halo_copies(up)[0].wait_recv()

    edge[0:16, :] = tb[0:EDGE, :]
    edge[16:32, :] = tb[EDGE + TOK :, :]
    phase(1 - hi, False)

    @pl.loop(0, 2)
    def _(i):
        j = (1 - hi) * 2 + i
        prepare(j)
        for d in range(2):
            scan_in(j, d)

    for h in range(2):

        @pl.when(hi == h)
        def _(h=h):
            scan_in(3 * h, h)

    row8 = lax.broadcasted_iota(jnp.int32, (8, 128), 0)
    shrink = jnp.exp2(tot_s[...])
    whole = jnp.exp2(tot_s[0:1, :] + tot_s[1:2, :] + tot_s[2:3, :] + tot_s[3:4, :])
    for g in range(8):
        tail = jnp.zeros((8, 128), F32)
        for d in range(2):
            base = d * 16 + 2 * g
            decay = expand(whole, base)
            high = decay.astype(BF).astype(F32)
            tail = jnp.where(row8 == 2 * d, high, tail)
            tail = jnp.where(row8 == 2 * d + 1, decay - high, tail)
            order = range(NBLK) if d == 0 else range(NBLK - 1, -1, -1)
            state = None
            for j in order:
                new = upd[d, j, :, lanes(g)]
                if state is None:
                    state = new
                else:
                    start[d, j, :, lanes(g)] = state.astype(BF)
                    state = state * expand(shrink[j : j + 1], base) + new
            state = state.astype(BF)
            for r in range(4):
                msg[g * 4 + r, d * 32 : d * 32 + 32] = state[r * 32 : r * 32 + 32]
        for r in range(4):
            msg[g * 4 + r, 64:72] = tail.astype(BF)

    def everywhere(src, dst, send, recv):
        copies = []
        for i, peer in enumerate(peers):
            copy = remote(src.at[peer], dst.at[frame], send.at[i], recv.at[i], dev(peer, row))
            copy.start()
            copies.append(copy)
        dst[frame] = src[frame]
        return copies

    there = everywhere(msg, got, a_s, a_r)

    @pl.loop(0, NBLK)
    def _(i):
        intra(i)

    for copy in there:
        copy.wait_recv()
    for d in range(2):
        state = jnp.zeros((32, 128), F32)
        for g in range(FRAMES) if d == 0 else reversed(range(FRAMES)):
            ret[g, d * 32 : d * 32 + 32] = state.astype(BF)
            tail = got[g, 64:72].astype(F32)
            decay = tail[2 * d : 2 * d + 1] + tail[2 * d + 1 : 2 * d + 2]
            state = decay * state + got[g, d * 32 : d * 32 + 32].astype(F32)
    back = everywhere(ret, inc, b_s, b_r)

    loads[5].wait()

    def put_gate(out, cols):
        gate[:, cols] = out.astype(BF)

    over(lambda: tb[EDGE : EDGE + TOK, :], wg, CH, 512, put_gate)

    def from_start(j, d):
        rows = block(j)
        grown = jnp.exp2(cum_s[rows, :])
        c = bc[rows, d * 256 + 128 : d * 256 + 256]
        for g in range(8):
            y_s[rows, lanes(g)] += expand(grown, d * 16 + 2 * g) * dot(c, start[d, j, :, lanes(g)])

    @pl.loop(0, NBLK - 1)
    def _(i):
        from_start(i + 1, 0)
        from_start(i, 1)

    zero = jnp.zeros((1, 128), F32)
    before, after = [zero], [zero]
    for j in range(NBLK - 1):
        before.append(before[-1] + tot_s[j : j + 1, :])
        after.append(after[-1] + tot_s[NBLK - 1 - j : NBLK - j, :])
    after = after[::-1]
    for j in range(NBLK):
        off_s[j : j + 1, :] = jnp.where(fwd_lane[0:1], before[j], after[j])

    @pl.loop(0, NBLK)
    def _(n):
        target = jnp.where(
            n == 0, corner, jnp.where(n == 1, across, jnp.where(n == 2, partner, row))
        )
        rows = block(target)
        ef = jnp.exp2(cum_s[rows, :] + off_s[pl.ds(target, 1), :])
        for g in range(8):
            open_g = silu(gate[rows, lanes(g)].astype(F32))
            y_s[rows, lanes(g)] = y_s[rows, lanes(g)] * open_g
            for d in range(2):
                ef_s[d, block(n), lanes(g)] = open_g * expand(ef, d * 16 + 2 * g)

    for copy in back:
        copy.wait_recv()
    for g in range(8):
        for r in range(4):
            for d in range(2):
                inc_m[d, r * 32 : r * 32 + 32, lanes(g)] = inc[g * 4 + r, d * 32 : d * 32 + 32]

    def gated_rows(n, target):
        rows = block(target)
        total = jnp.zeros((BLK, BLK), F32)
        for g in range(8):
            gated = y_s[rows, lanes(g)]
            for d in range(2):
                c = bc[rows, d * 256 + 128 : d * 256 + 256]
                gated = gated + ef_s[d, block(n), lanes(g)] * dot(c, inc_m[d, :, lanes(g)])
            total = total + gated * gated
            normed[block(n), lanes(g)] = (gated * gain_ref[:, lanes(g)]).astype(BF)
        sq[n] = jnp.broadcast_to(jnp.sum(total.T, axis=0, keepdims=True), (8, BLK))

    @pl.loop(0, 2)
    def _(n):
        gated_rows(n, jnp.where(n == 0, corner, across))

    loads[6].wait()
    ones, twos, threes = [], [], []

    def relay(k):
        ones[k].wait_recv()
        to_across[k] = (own[k] + from_partner[0, k].astype(F32)).astype(BF)
        copy = remote(
            to_across.at[k], from_across.at[k], f_s.at[NCOL + k], f_r.at[NCOL + k],
            dev(frame, across),
        )
        copy.start()
        twos.append(copy)

    for k in range(NCOL):
        cols = slice(k * COLS, (k + 1) * COLS)
        part = dot(normed[0:HALF, :], wo[:, cols])
        to_partner[0, k] = part[0:BLK].astype(BF)
        copy = remote(
            to_partner.at[0, k], from_partner.at[0, k], f_s.at[k], f_r.at[k], dev(frame, partner)
        )
        copy.start()
        ones.append(copy)
        own[k] = part[BLK:]
        if k >= LAG:
            relay(k - LAG)
    for k in range(NCOL - LAG, NCOL):
        relay(k)
    @pl.loop(2, 4)
    def _(n):
        gated_rows(n, jnp.where(n == 2, partner, row))

    sq_out[0] = sq[0]
    sq_out[1] = sq[2]
    sq_copy = remote(sq_out, sq_part, f_s.at[3 * NCOL], f_r.at[3 * NCOL], dev(frame, partner))
    sq_copy.start()
    for k in range(NCOL):
        cols = slice(k * COLS, (k + 1) * COLS)
        part = dot(normed[HALF:, :], wo[:, cols])
        to_partner[1, k] = part[0:BLK].astype(BF)
        copy = remote(
            to_partner.at[1, k], from_partner.at[1, k], f_s.at[2 * NCOL + k],
            f_r.at[2 * NCOL + k], dev(frame, partner),
        )
        copy.start()
        threes.append(copy)
        own[k] = part[BLK:]
    sq_copy.wait_recv()
    sq_cross[...] = sq[1] + sq_part[0]
    far_copy = remote(
        sq_cross, sq_far, f_s.at[3 * NCOL + 1], f_r.at[3 * NCOL + 1], dev(frame, across)
    )
    far_copy.start()
    for k in range(NCOL):
        threes[k].wait_recv()
        own[k] = own[k] + from_partner[1, k].astype(F32)
    far_copy.wait_recv()
    mean = (sq[3] + sq_part[1] + sq_far[...]) * (1.0 / D_INNER)
    scale = jnp.broadcast_to(lax.rsqrt(mean + 1e-05)[0:1], (BLK, BLK)).T[:, 0:1]
    for k in range(NCOL):
        cols = slice(k * COLS, (k + 1) * COLS)
        twos[k].wait_recv()
        out_ref[:, cols] = (scale * (own[k] + from_across[k].astype(F32))).astype(BF)

    near.wait_send()
    for i in range(CHUNKS):
        cross(i, row, hi).wait_send()
        forward(i).wait_send()
    for up, flag in ((True, to_next), (False, to_prev)):

        @pl.when(flag)
        def _(up=up):
            for copy in halo_copies(up):
                copy.wait_send()

    for copy in there + back + ones + twos + threes + [sq_copy, far_copy]:
        copy.wait_send()


def layer(*operands):
    dma = pltpu.SemaphoreType.DMA
    vmem = pltpu.VMEM
    return pl.pallas_call(
        layer_body,
        name="layer",
        out_shape=jax.ShapeDtypeStruct((BLK, D), BF),
        in_specs=[ANY] * 6 + [VM] * 5,
        out_specs=VM,
        scratch_shapes=[
            vmem((TOK + 2 * EDGE, D), BF), vmem((32, D), BF),
            vmem((D, CH), BF), vmem((D, CH), BF), vmem((D, 512), BF), vmem((128, D), BF),
            vmem((CH, D), BF), vmem((8, 128), F32), vmem((TOK, CH), BF), vmem((TOK, 512), BF),
            vmem((TOK + 2 * EDGE, CH), F32),
            vmem((2, TOK, CH), BF),
            vmem((2, NBLK, 128, CH), BF), vmem((2, NBLK, 128, CH), F32), vmem((BLK, CH), BF),
            vmem((TOK, 128), F32), vmem((TOK, 128), F32), vmem((8, 128), F32),
            vmem((TOK, CH), F32), vmem((2, TOK, CH), F32), vmem((8, 128), F32),
            vmem((FRAMES, MSG, 128), BF), vmem((FRAMES, MSG, 128), BF),
            vmem((FRAMES, 64, 128), BF), vmem((FRAMES, 64, 128), BF), vmem((2, 128, CH), BF),
            vmem((TOK, CH), BF), vmem((4, 8, 128), F32),
            vmem((2, NCOL, BLK, COLS), BF), vmem((2, NCOL, BLK, COLS), BF),
            vmem((NCOL, BLK, COLS), BF), vmem((NCOL, BLK, COLS), BF),
            vmem((NCOL, BLK, COLS), F32),
            vmem((2, 8, 128), F32), vmem((2, 8, 128), F32), vmem((8, 128), F32),
            vmem((8, 128), F32),
            dma((7,)), dma((2 * CHUNKS + 9,)), dma((2 * CHUNKS + 3,)),
            dma((PEERS,)), dma((PEERS,)), dma((PEERS,)), dma((PEERS,)),
            dma((3 * NCOL + 2,)), dma((3 * NCOL + 2,)),
        ],
        compiler_params=pltpu.CompilerParams(
            collective_id=0, has_side_effects=True, vmem_limit_bytes=62 * 1024 * 1024
        ),
    )(*operands)


def per_device(
    tokens, w_gate, w_value, w_state_proj, w_step, step_bias, decay_rate, conv_taps,
    skip_gain, norm_gain, w_out,
):
    out = layer(
        tokens[0], w_gate, w_value, w_state_proj, jnp.swapaxes(w_step, 1, 2), w_out,
        step_bias, decay_rate, skip_gain, conv_taps, norm_gain[None, :],
    )
    return out[None]


def solution(mesh):
    in_specs = (
        P("frame", "row", None), P(None, "row"), P(None, "row"), P(), P(None, None, "row"),
        P(None, "row"), P(None, "row"), P(None, None, "row"), P(None, "row"), P("row"),
        P("row", None),
    )
    return jax.shard_map(
        per_device, mesh=mesh, in_specs=in_specs, out_specs=P("frame", "row", None),
        check_vma=False,
    )
```

```python
import jax
import jax.numpy as jnp
from jax import lax
from jax.experimental import pallas as pl
from jax.experimental.pallas import tpu as pltpu
from jax.sharding import PartitionSpec as P

BF = jnp.bfloat16
F32 = jnp.float32
FRAMES = 32
TOK = 512
BLK = 128
NBLK = 4
CH = 1024
D = 2048
HALF = 256
HALO = 8
LOG2E = 1.4426950408889634
D_INNER = 4096
VM = pl.BlockSpec(memory_space=pltpu.VMEM)
ANY = pl.BlockSpec(memory_space=pl.ANY)
MSG = 72


def silu(x):
    return 0.5 * x * (1.0 + jnp.tanh(0.5 * x))


def dot(a, b):
    return jnp.dot(a, b, preferred_element_type=F32)


def dev(frame, row):
    return {"frame": frame, "row": row}


def place():
    frame, row = lax.axis_index("frame"), lax.axis_index("row")
    core = lax.rem(row, 2)
    return frame, row, core, lax.div(row, 2)


def remote(src, dst, send, recv, target):
    return pltpu.make_async_remote_copy(src, dst, send, recv, device_id=target)


CHUNKS = 4
CROWS = 128 // CHUNKS
HALF_BLK = 64
EDGE = 16
COLS = 512
LAG = 2
NCOL = D // COLS
PEERS = FRAMES - 1
STEPS = sorted(
    ((dx, dy, dz) for dx in range(4) for dy in range(4) for dz in range(2) if dx + dy + dz),
    key=lambda s: -(min(s[0], 4 - s[0]) + min(s[1], 4 - s[1]) + s[2]),
)


def expand(values, base):
    lane = lax.broadcasted_iota(jnp.int32, (1, 128), 1)
    return jnp.where(lane < 64, values[:, base : base + 1], values[:, base + 1 : base + 2])


def lanes(group):
    return slice(group * 128, group * 128 + 128)


def block(j, count=BLK, shift=0):
    return pl.ds(pl.multiple_of(j * BLK + shift, 16), count)


def layer_body(
    tok_ref, wg_ref, wv_ref, ws_ref, wt_ref, wo_ref,
    bias_ref, rate_ref, skip_ref, taps_ref, gain_ref,
    out_ref,
    tb, edge, wg, wv, ws, wt, wo, par, gate, bc,
    xp, xs, start, upd, car, cum_s, dt_s, tot_s, y_s, ef_s, off_s,
    msg, got, ret, inc, inc_m,
    normed, sq, to_partner, from_partner, to_across, from_across, own,
    sq_out, sq_part, sq_cross, sq_far,
    w_sem, g_s, g_r, a_s, a_r, b_s, b_r, f_s, f_r,
):
    frame, row, core, hi = place()
    partner = row + 1 - 2 * core
    across = lax.rem(row + 2, 4)
    corner = lax.rem(partner + 2, 4)
    fx, fy, fz = lax.div(frame, 8), lax.rem(lax.div(frame, 2), 4), lax.rem(frame, 2)
    peers = [
        lax.rem(fx + dx, 4) * 8 + lax.rem(fy + dy, 4) * 2 + lax.rem(fz + dz, 2)
        for dx, dy, dz in STEPS
    ]
    first, final = frame == 0, frame == FRAMES - 1

    mine = pl.ds(pl.multiple_of(EDGE + row * BLK, 16), BLK)
    loads = []
    for i, (src, dst) in enumerate((
        (tok_ref, tb.at[mine]), (wv_ref, wv), (ws_ref, ws),
        (wt_ref.at[0], wt.at[0:16]), (wt_ref.at[1], wt.at[16:32]),
        (wg_ref, wg), (wo_ref, wo),
    )):
        copy = pltpu.make_async_copy(src, dst, w_sem.at[i])
        copy.start()
        loads.append(copy)
    tb[0:EDGE, :] = jnp.zeros((EDGE, D), BF)
    tb[EDGE + TOK :, :] = jnp.zeros((EDGE, D), BF)
    barrier = pltpu.get_barrier_semaphore()
    for peer in (partner, across):
        pl.semaphore_signal(barrier, inc=1, device_id=dev(frame, peer))
    for peer in peers:
        pl.semaphore_signal(barrier, inc=1, device_id=dev(peer, row))

    @pl.when(jnp.logical_not(first))
    def _():
        pl.semaphore_signal(barrier, inc=1, device_id=dev(frame - 1, 3))

    @pl.when(jnp.logical_not(final))
    def _():
        pl.semaphore_signal(barrier, inc=1, device_id=dev(frame + 1, 0))

    to_next = jnp.logical_and(row == 3, jnp.logical_not(final))
    to_prev = jnp.logical_and(row == 0, jnp.logical_not(first))
    wt[32:128, :] = jnp.zeros((96, D), BF)
    par[...] = jnp.zeros_like(par)
    for i, ref in enumerate((bias_ref, rate_ref, skip_ref)):
        for d in range(2):
            par[i : i + 1, d * 16 : d * 16 + 16] = ref[d : d + 1, :]
    loads[0].wait()
    pl.semaphore_wait(
        barrier, 2 + PEERS + jnp.where(jnp.logical_or(to_next, to_prev), 4, 0)
    )

    def chunk_rows(sender, i, side):
        at = jnp.where(side == 1, i % 2, 1 - i % 2) * CROWS + sender * HALF_BLK
        source = 1 + side if i < 2 else 3 * side
        return pl.ds(pl.multiple_of(EDGE + source * BLK + at, 16), CROWS)

    def cross(i, side):
        rows = chunk_rows(core, i, side)
        return remote(tb.at[rows], tb.at[rows], g_s.at[i], g_r.at[i], dev(frame, across))

    def over_chip(i, sender):
        rows = chunk_rows(sender, i, 1 - hi)
        return remote(
            tb.at[rows], tb.at[rows], g_s.at[CHUNKS + i], g_r.at[CHUNKS + i], dev(frame, partner)
        )

    def forward(i):
        return over_chip(i, core)

    def forwarded(i):
        return over_chip(i, 1 - core)

    def pass_on(i):
        cross(i, 1 - hi).wait_recv()
        forward(i).start()

    near = remote(
        tb.at[mine], tb.at[mine], g_s.at[2 * CHUNKS], g_r.at[2 * CHUNKS], dev(frame, partner)
    )

    def halo_copies(up):
        src = tb.at[pl.ds(pl.multiple_of(EDGE + row * BLK + (BLK - HALO if up else 0), HALO), HALO)]
        dst = tb.at[pl.ds(EDGE - HALO if up else EDGE + TOK, HALO)]
        base = 2 * CHUNKS + 1 + (0 if up else 4)
        return [
            remote(
                src, dst, g_s.at[base + r], g_r.at[2 * CHUNKS + 1 + (0 if up else 1)],
                dev(frame + 1 if up else frame - 1, r),
            )
            for r in range(4)
        ]

    near.start()

    @pl.when(core == 1 - hi)
    def _():
        cross(0, hi).start()
        cross(1, hi).start()

    for up, flag in ((True, to_next), (False, to_prev)):

        @pl.when(flag)
        def _(up=up):
            for copy in halo_copies(up):
                copy.start()

    def over(read, weight, columns, width, store):
        @pl.loop(0, columns // width)
        def _(n):
            cols = pl.ds(pl.multiple_of(n * width, width), width)
            store(dot(read(), weight[:, cols]), cols)

    def phase(base, count, waits, ends):
        rows = pl.ds(pl.multiple_of(base, 16), count)
        rows_x = pl.ds(pl.multiple_of(EDGE + base, 16), count)

        def read():
            return tb[rows_x, :]

        def read_x():
            return jnp.concatenate([read(), edge[...]], axis=0) if ends else read()

        def put_x(out, cols):
            out = out.astype(BF).astype(F32)
            xp[rows_x, cols] = out[:count]
            if ends:
                xp[0:EDGE, cols] = out[count : count + EDGE]
                xp[EDGE + TOK :, cols] = out[count + EDGE :]

        def put_bc(out, cols):
            bc[rows, cols] = out.astype(BF)

        if waits:
            loads[1].wait()
        over(read_x, wv, CH, 512, put_x)
        if waits:
            loads[2].wait()
        over(read, ws, 512, 512, put_bc)
        if waits:
            loads[3].wait()
            loads[4].wait()
        raw = lax.dot_general(
            read(), wt[...], (((1,), (1,)), ((), ())), preferred_element_type=F32
        ).astype(BF).astype(F32) + par[0:1, :]
        dt_s[rows, :] = jnp.maximum(raw, 0.0) + jnp.log1p(jnp.exp(-jnp.abs(raw)))

    row_i = lax.broadcasted_iota(jnp.int32, (BLK, BLK), 0)
    col_i = lax.broadcasted_iota(jnp.int32, (BLK, BLK), 1)
    lower, upper = row_i >= col_i, col_i >= row_i
    fwd_lane = col_i < 16

    def prepare(j):
        rows = block(j)
        part = dt_s[rows, :] * (par[1:2, :] * -LOG2E)
        high = part.astype(BF)
        rest = part - high.astype(F32)
        mid = rest.astype(BF)
        low = (rest - mid.astype(F32)).astype(BF)
        tri = lower.astype(BF)
        cum = dot(tri, high) + (dot(tri, mid) + dot(tri, low))
        total = cum[BLK - 1 : BLK]
        cum_s[rows, :] = jnp.where(fwd_lane, cum, (total - cum) + part)
        tot_s[pl.ds(j, 1), :] = total

    def scan_in(j, d):
        size = BLK + 2 * EDGE
        rows = block(j)
        fade = jnp.exp2(tot_s[pl.ds(j, 1), :] - cum_s[rows, :]) * dt_s[rows, :]
        bt = bc[rows, d * 256 : d * 256 + 128].astype(F32).T.astype(BF)
        for g in range(8):
            window = xp[block(j, size), lanes(g)]
            acc = None
            for k in range(4):
                o = 3 - k if d else k - 3
                moved = pltpu.roll(window, (-o) % size, 0) if o else window
                term = taps_ref[d, k : k + 1, lanes(g)] * moved[EDGE : EDGE + BLK]
                acc = term if acc is None else acc + term
            x = silu(acc).astype(BF)
            xs[d, rows, lanes(g)] = x
            carried = (x.astype(F32) * expand(fade, d * 16 + 2 * g)).astype(BF)
            upd[d, pl.ds(j, 1), :, lanes(g)] = dot(bt, carried)[None]

    def intra(j):
        rows = block(j)
        cum = cum_s[rows, :]
        cum_t, dt_t = cum.T, dt_s[rows, :].T
        skip = par[2:3, :]
        scores = []
        for d in range(2):
            s = lax.dot_general(
                bc[rows, d * 256 + 128 : d * 256 + 256], bc[rows, d * 256 : d * 256 + 128],
                (((1,), (1,)), ((), ())), preferred_element_type=F32,
            )
            scores.append(jnp.where(lower if d == 0 else upper, s, 0.0))
        for g in range(8):
            values = jnp.concatenate([xs[0, rows, lanes(g)], xs[1, rows, lanes(g)]], axis=0)
            outs = []
            for k in range(2):
                w = []
                for d in range(2):
                    n = d * 16 + 2 * g + k
                    gap = jnp.minimum(cum[:, n : n + 1] - cum_t[n : n + 1, :], 0.0)
                    w.append((scores[d] * jnp.exp2(gap) * dt_t[n : n + 1, :]).astype(BF))
                outs.append(dot(jnp.concatenate(w, axis=1), values))
            y = jnp.where(col_i < 64, outs[0], outs[1])
            for d in range(2):
                y = y + expand(skip, d * 16 + 2 * g) * xs[d, rows, lanes(g)].astype(F32)
            y_s[rows, lanes(g)] = y

    near.wait_recv()

    @pl.when(core != 1 - hi)
    def _():
        cross(0, hi).start()
        cross(1, hi).start()

    cross(2, hi).start()
    cross(3, hi).start()
    phase(hi * HALF, HALF, True, False)
    @pl.when(core == hi)
    def _():
        pass_on(0)

    @pl.when(core != hi)
    def _():
        forwarded(0).wait_recv()

    beside = pl.ds(pl.multiple_of(jnp.where(hi == 0, EDGE + HALF, HALF), 16), EDGE)

    def put_edge(out, cols):
        xp[beside, cols] = out.astype(BF).astype(F32)

    over(lambda: tb[beside, :], wv, CH, 512, put_edge)

    prepare(hi * 2)
    prepare(hi * 2 + 1)
    scan_in(1 + hi, 0)

    @pl.when(core != hi)
    def _():
        pass_on(0)

    pass_on(1)
    scan_in(1 + hi, 1)
    for h in range(2):

        @pl.when(hi == h)
        def _(h=h):
            scan_in(3 * h, 1 - h)

    @pl.when(core == hi)
    def _():
        forwarded(0).wait_recv()

    forwarded(1).wait_recv()
    phase((2 - hi) * BLK, BLK, False, False)
    prepare(2 - hi)
    pass_on(2)
    for h in range(2):

        @pl.when(hi == h)
        def _(h=h):
            scan_in(2 - h, h)

    pass_on(3)
    forwarded(2).wait_recv()
    forwarded(3).wait_recv()
    for up, flag in ((True, first), (False, final)):

        @pl.when(jnp.logical_not(flag))
        def _(up=up):
            halo_copies(up)[0].wait_recv()

    edge[0:16, :] = tb[0:EDGE, :]
    edge[16:32, :] = tb[EDGE + TOK :, :]
    phase((1 - hi) * 3 * BLK, BLK, False, True)
    prepare((1 - hi) * 3)
    for d in range(2):
        scan_in((1 - hi) * 3, d)
    for h in range(2):

        @pl.when(hi == h)
        def _(h=h):
            scan_in(2 - h, 1 - h)
            scan_in(3 * h, h)

    row8 = lax.broadcasted_iota(jnp.int32, (8, 128), 0)
    shrink = jnp.exp2(tot_s[...])
    whole = jnp.exp2(tot_s[0:1, :] + tot_s[1:2, :] + tot_s[2:3, :] + tot_s[3:4, :])
    for g in range(8):
        tail = jnp.zeros((8, 128), F32)
        for d in range(2):
            base = d * 16 + 2 * g
            decay = expand(whole, base)
            high = decay.astype(BF).astype(F32)
            tail = jnp.where(row8 == 2 * d, high, tail)
            tail = jnp.where(row8 == 2 * d + 1, decay - high, tail)
            order = range(NBLK) if d == 0 else range(NBLK - 1, -1, -1)
            state = None
            for j in order:
                new = upd[d, j, :, lanes(g)]
                if state is None:
                    state = new
                else:
                    start[d, j, :, lanes(g)] = state.astype(BF)
                    state = state * expand(shrink[j : j + 1], base) + new
            state = state.astype(BF)
            for r in range(4):
                msg[g * 4 + r, d * 32 : d * 32 + 32] = state[r * 32 : r * 32 + 32]
        for r in range(4):
            msg[g * 4 + r, 64:72] = tail.astype(BF)

    def everywhere(src, dst, send, recv):
        copies = []
        for i, peer in enumerate(peers):
            copy = remote(src.at[peer], dst.at[frame], send.at[i], recv.at[i], dev(peer, row))
            copy.start()
            copies.append(copy)
        dst[frame] = src[frame]
        return copies

    there = everywhere(msg, got, a_s, a_r)

    @pl.loop(0, NBLK)
    def _(i):
        intra(i)

    loads[5].wait()

    def put_gate(out, cols):
        gate[:, cols] = out.astype(BF)

    over(lambda: tb[EDGE : EDGE + TOK, :], wg, CH, 512, put_gate)

    for copy in there:
        copy.wait_recv()
    for d in range(2):
        state = jnp.zeros((32, 128), F32)
        for g in range(FRAMES) if d == 0 else reversed(range(FRAMES)):
            ret[g, d * 32 : d * 32 + 32] = state.astype(BF)
            tail = got[g, 64:72].astype(F32)
            decay = tail[2 * d : 2 * d + 1] + tail[2 * d + 1 : 2 * d + 2]
            state = decay * state + got[g, d * 32 : d * 32 + 32].astype(F32)
    back = everywhere(ret, inc, b_s, b_r)

    def from_start(j, d):
        rows = block(j)
        grown = jnp.exp2(cum_s[rows, :])
        c = bc[rows, d * 256 + 128 : d * 256 + 256]
        for g in range(8):
            y_s[rows, lanes(g)] += expand(grown, d * 16 + 2 * g) * dot(c, start[d, j, :, lanes(g)])

    @pl.loop(0, NBLK - 1)
    def _(i):
        from_start(i + 1, 0)
        from_start(i, 1)

    zero = jnp.zeros((1, 128), F32)
    before, after = [zero], [zero]
    for j in range(NBLK - 1):
        before.append(before[-1] + tot_s[j : j + 1, :])
        after.append(after[-1] + tot_s[NBLK - 1 - j : NBLK - j, :])
    after = after[::-1]
    for j in range(NBLK):
        off_s[j : j + 1, :] = jnp.where(fwd_lane[0:1], before[j], after[j])

    @pl.loop(0, NBLK)
    def _(n):
        target = jnp.where(
            n == 0, corner, jnp.where(n == 1, across, jnp.where(n == 2, partner, row))
        )
        rows = block(target)
        ef = jnp.exp2(cum_s[rows, :] + off_s[pl.ds(target, 1), :])
        for g in range(8):
            open_g = silu(gate[rows, lanes(g)].astype(F32))
            y_s[rows, lanes(g)] = y_s[rows, lanes(g)] * open_g
            for d in range(2):
                ef_s[d, block(n), lanes(g)] = open_g * expand(ef, d * 16 + 2 * g)

    for copy in back:
        copy.wait_recv()
    for g in range(8):
        for r in range(4):
            for d in range(2):
                inc_m[d, r * 32 : r * 32 + 32, lanes(g)] = inc[g * 4 + r, d * 32 : d * 32 + 32]

    def gated_rows(n, target):
        rows = block(target)
        total = jnp.zeros((BLK, BLK), F32)
        for g in range(8):
            gated = y_s[rows, lanes(g)]
            for d in range(2):
                c = bc[rows, d * 256 + 128 : d * 256 + 256]
                gated = gated + ef_s[d, block(n), lanes(g)] * dot(c, inc_m[d, :, lanes(g)])
            total = total + gated * gated
            normed[block(n), lanes(g)] = (gated * gain_ref[:, lanes(g)]).astype(BF)
        sq[n] = jnp.broadcast_to(jnp.sum(total.T, axis=0, keepdims=True), (8, BLK))

    @pl.loop(0, 2)
    def _(n):
        gated_rows(n, jnp.where(n == 0, corner, across))

    loads[6].wait()
    ones, twos, threes = [], [], []

    def relay(k):
        ones[k].wait_recv()
        to_across[k] = (own[k] + from_partner[0, k].astype(F32)).astype(BF)
        copy = remote(
            to_across.at[k], from_across.at[k], f_s.at[NCOL + k], f_r.at[NCOL + k],
            dev(frame, across),
        )
        copy.start()
        twos.append(copy)

    for k in range(NCOL):
        cols = slice(k * COLS, (k + 1) * COLS)
        part = dot(normed[0:HALF, :], wo[:, cols])
        to_partner[0, k] = part[0:BLK].astype(BF)
        copy = remote(
            to_partner.at[0, k], from_partner.at[0, k], f_s.at[k], f_r.at[k], dev(frame, partner)
        )
        copy.start()
        ones.append(copy)
        own[k] = part[BLK:]
        if k >= LAG:
            relay(k - LAG)
    for k in range(NCOL - LAG, NCOL):
        relay(k)
    @pl.loop(2, 4)
    def _(n):
        gated_rows(n, jnp.where(n == 2, partner, row))

    sq_out[0] = sq[0]
    sq_out[1] = sq[2]
    sq_copy = remote(sq_out, sq_part, f_s.at[3 * NCOL], f_r.at[3 * NCOL], dev(frame, partner))
    sq_copy.start()
    for k in range(NCOL):
        cols = slice(k * COLS, (k + 1) * COLS)
        part = dot(normed[HALF:, :], wo[:, cols])
        to_partner[1, k] = part[0:BLK].astype(BF)
        copy = remote(
            to_partner.at[1, k], from_partner.at[1, k], f_s.at[2 * NCOL + k],
            f_r.at[2 * NCOL + k], dev(frame, partner),
        )
        copy.start()
        threes.append(copy)
        own[k] = part[BLK:]
    sq_copy.wait_recv()
    sq_cross[...] = sq[1] + sq_part[0]
    far_copy = remote(
        sq_cross, sq_far, f_s.at[3 * NCOL + 1], f_r.at[3 * NCOL + 1], dev(frame, across)
    )
    far_copy.start()
    for k in range(NCOL):
        threes[k].wait_recv()
        own[k] = own[k] + from_partner[1, k].astype(F32)
    far_copy.wait_recv()
    mean = (sq[3] + sq_part[1] + sq_far[...]) * (1.0 / D_INNER)
    scale = jnp.broadcast_to(lax.rsqrt(mean + 1e-05)[0:1], (BLK, BLK)).T[:, 0:1]
    for k in range(NCOL):
        cols = slice(k * COLS, (k + 1) * COLS)
        twos[k].wait_recv()
        out_ref[:, cols] = (scale * (own[k] + from_across[k].astype(F32))).astype(BF)

    near.wait_send()
    for i in range(CHUNKS):
        cross(i, hi).wait_send()
        forward(i).wait_send()
    for up, flag in ((True, to_next), (False, to_prev)):

        @pl.when(flag)
        def _(up=up):
            for copy in halo_copies(up):
                copy.wait_send()

    for copy in there + back + ones + twos + threes + [sq_copy, far_copy]:
        copy.wait_send()


def layer(*operands):
    dma = pltpu.SemaphoreType.DMA
    vmem = pltpu.VMEM
    return pl.pallas_call(
        layer_body,
        name="layer",
        out_shape=jax.ShapeDtypeStruct((BLK, D), BF),
        in_specs=[ANY] * 6 + [VM] * 5,
        out_specs=VM,
        scratch_shapes=[
            vmem((TOK + 2 * EDGE, D), BF), vmem((32, D), BF),
            vmem((D, CH), BF), vmem((D, CH), BF), vmem((D, 512), BF), vmem((128, D), BF),
            vmem((CH, D), BF), vmem((8, 128), F32), vmem((TOK, CH), BF), vmem((TOK, 512), BF),
            vmem((TOK + 2 * EDGE, CH), F32),
            vmem((2, TOK, CH), BF),
            vmem((2, NBLK, 128, CH), BF), vmem((2, NBLK, 128, CH), F32), vmem((BLK, CH), BF),
            vmem((TOK, 128), F32), vmem((TOK, 128), F32), vmem((8, 128), F32),
            vmem((TOK, CH), F32), vmem((2, TOK, CH), F32), vmem((8, 128), F32),
            vmem((FRAMES, MSG, 128), BF), vmem((FRAMES, MSG, 128), BF),
            vmem((FRAMES, 64, 128), BF), vmem((FRAMES, 64, 128), BF), vmem((2, 128, CH), BF),
            vmem((TOK, CH), BF), vmem((4, 8, 128), F32),
            vmem((2, NCOL, BLK, COLS), BF), vmem((2, NCOL, BLK, COLS), BF),
            vmem((NCOL, BLK, COLS), BF), vmem((NCOL, BLK, COLS), BF),
            vmem((NCOL, BLK, COLS), F32),
            vmem((2, 8, 128), F32), vmem((2, 8, 128), F32), vmem((8, 128), F32),
            vmem((8, 128), F32),
            dma((7,)), dma((2 * CHUNKS + 9,)), dma((2 * CHUNKS + 3,)),
            dma((PEERS,)), dma((PEERS,)), dma((PEERS,)), dma((PEERS,)),
            dma((3 * NCOL + 2,)), dma((3 * NCOL + 2,)),
        ],
        compiler_params=pltpu.CompilerParams(
            collective_id=0, has_side_effects=True, vmem_limit_bytes=62 * 1024 * 1024
        ),
    )(*operands)


def per_device(
    tokens, w_gate, w_value, w_state_proj, w_step, step_bias, decay_rate, conv_taps,
    skip_gain, norm_gain, w_out,
):
    out = layer(
        tokens[0], w_gate, w_value, w_state_proj, jnp.swapaxes(w_step, 1, 2), w_out,
        step_bias, decay_rate, skip_gain, conv_taps, norm_gain[None, :],
    )
    return out[None]


def solution(mesh):
    in_specs = (
        P("frame", "row", None), P(None, "row"), P(None, "row"), P(), P(None, None, "row"),
        P(None, "row"), P(None, "row"), P(None, None, "row"), P(None, "row"), P("row"),
        P("row", None),
    )
    return jax.shard_map(
        per_device, mesh=mesh, in_specs=in_specs, out_specs=P("frame", "row", None),
        check_vma=False,
    )
```

```python
import jax
import jax.numpy as jnp
from jax import lax
from jax.experimental import pallas as pl
from jax.experimental.pallas import tpu as pltpu
from jax.sharding import PartitionSpec as P

BF = jnp.bfloat16
F32 = jnp.float32
FRAMES = 32
TOK = 512
BLK = 128
NBLK = 4
CH = 1024
D = 2048
HALF = 256
HALO = 8
LOG2E = 1.4426950408889634
D_INNER = 4096
VM = pl.BlockSpec(memory_space=pltpu.VMEM)
ANY = pl.BlockSpec(memory_space=pl.ANY)
MSG = 72


def silu(x):
    return 0.5 * x * (1.0 + jnp.tanh(0.5 * x))


def dot(a, b):
    return jnp.dot(a, b, preferred_element_type=F32)


def dev(frame, row):
    return {"frame": frame, "row": row}


def place():
    frame, row = lax.axis_index("frame"), lax.axis_index("row")
    core = lax.rem(row, 2)
    return frame, row, core, lax.div(row, 2)


def remote(src, dst, send, recv, target):
    return pltpu.make_async_remote_copy(src, dst, send, recv, device_id=target)


CHUNKS = 4
CROWS = 128 // CHUNKS
HALF_BLK = 64
EDGE = 16
COLS = 512
LAG = 1
NCOL = D // COLS
PEERS = FRAMES - 1
STEPS = sorted(
    ((dx, dy, dz) for dx in range(4) for dy in range(4) for dz in range(2) if dx + dy + dz),
    key=lambda s: -(min(s[0], 4 - s[0]) + min(s[1], 4 - s[1]) + s[2]),
)


def expand(values, base):
    lane = lax.broadcasted_iota(jnp.int32, (1, 128), 1)
    return jnp.where(lane < 64, values[:, base : base + 1], values[:, base + 1 : base + 2])


def lanes(group):
    return slice(group * 128, group * 128 + 128)


def block(j, count=BLK, shift=0):
    return pl.ds(pl.multiple_of(j * BLK + shift, 16), count)


def layer_body(
    tok_ref, wg_ref, wv_ref, ws_ref, wt_ref, wo_ref,
    bias_in, rate_in, skip_in, taps_in, gain_in,
    out_ref,
    bias_ref, rate_ref, skip_ref, taps_ref, gain_ref,
    tb, edge, wg, wv, ws, wt, wo, par, gate, bc,
    xp, xs, start, upd, car, cum_s, dt_s, tot_s, y_s, ef_s, off_s,
    msg, got, ret, inc, inc_m,
    normed, sq, to_partner, from_partner, to_across, from_across, own,
    sq_out, sq_part, sq_cross, sq_far,
    w_sem, g_s, g_r, a_s, a_r, b_s, b_r, f_s, f_r,
):
    frame, row, core, hi = place()
    partner = row + 1 - 2 * core
    across = lax.rem(row + 2, 4)
    corner = lax.rem(partner + 2, 4)
    fx, fy, fz = lax.div(frame, 8), lax.rem(lax.div(frame, 2), 4), lax.rem(frame, 2)
    peers = [
        lax.rem(fx + dx, 4) * 8 + lax.rem(fy + dy, 4) * 2 + lax.rem(fz + dz, 2)
        for dx, dy, dz in STEPS
    ]
    first, final = frame == 0, frame == FRAMES - 1

    mine = pl.ds(pl.multiple_of(EDGE + row * BLK, 16), BLK)
    loads = []
    for i, (src, dst) in enumerate((
        (tok_ref, tb.at[mine]), (bias_in, bias_ref), (rate_in, rate_ref), (skip_in, skip_ref),
        (wv_ref, wv), (ws_ref, ws), (wt_ref.at[0], wt.at[0:16]), (wt_ref.at[1], wt.at[16:32]),
        (taps_in, taps_ref), (gain_in, gain_ref), (wg_ref, wg), (wo_ref, wo),
    )):
        copy = pltpu.make_async_copy(src, dst, w_sem.at[i])
        copy.start()
        loads.append(copy)
    tb[0:EDGE, :] = jnp.zeros((EDGE, D), BF)
    tb[EDGE + TOK :, :] = jnp.zeros((EDGE, D), BF)
    barrier = pltpu.get_barrier_semaphore()
    for peer in (partner, across):
        pl.semaphore_signal(barrier, inc=1, device_id=dev(frame, peer))
    for peer in peers:
        pl.semaphore_signal(barrier, inc=1, device_id=dev(peer, row))

    @pl.when(jnp.logical_not(first))
    def _():
        pl.semaphore_signal(barrier, inc=1, device_id=dev(frame - 1, 3))

    @pl.when(jnp.logical_not(final))
    def _():
        pl.semaphore_signal(barrier, inc=1, device_id=dev(frame + 1, 0))

    to_next = jnp.logical_and(row == 3, jnp.logical_not(final))
    to_prev = jnp.logical_and(row == 0, jnp.logical_not(first))
    wt[32:128, :] = jnp.zeros((96, D), BF)
    par[...] = jnp.zeros_like(par)
    loads[0].wait()
    pl.semaphore_wait(
        barrier, 2 + PEERS + jnp.where(jnp.logical_or(to_next, to_prev), 4, 0)
    )

    def chunk_rows(sender, i, side):
        at = jnp.where(side == 1, i % 2, 1 - i % 2) * CROWS + sender * HALF_BLK
        source = 1 + side if i < 2 else 3 * side
        return pl.ds(pl.multiple_of(EDGE + source * BLK + at, 16), CROWS)

    def cross(i, side):
        rows = chunk_rows(core, i, side)
        return remote(tb.at[rows], tb.at[rows], g_s.at[i], g_r.at[i], dev(frame, across))

    def over_chip(i, sender):
        rows = chunk_rows(sender, i, 1 - hi)
        return remote(
            tb.at[rows], tb.at[rows], g_s.at[CHUNKS + i], g_r.at[CHUNKS + i], dev(frame, partner)
        )

    def forward(i):
        return over_chip(i, core)

    def forwarded(i):
        return over_chip(i, 1 - core)

    def pass_on(i):
        cross(i, 1 - hi).wait_recv()
        forward(i).start()

    near = remote(
        tb.at[mine], tb.at[mine], g_s.at[2 * CHUNKS], g_r.at[2 * CHUNKS], dev(frame, partner)
    )

    def halo_copies(up):
        src = tb.at[pl.ds(pl.multiple_of(EDGE + row * BLK + (BLK - HALO if up else 0), HALO), HALO)]
        dst = tb.at[pl.ds(EDGE - HALO if up else EDGE + TOK, HALO)]
        base = 2 * CHUNKS + 1 + (0 if up else 4)
        return [
            remote(
                src, dst, g_s.at[base + r], g_r.at[2 * CHUNKS + 1 + (0 if up else 1)],
                dev(frame + 1 if up else frame - 1, r),
            )
            for r in range(4)
        ]

    near.start()

    @pl.when(core == 1 - hi)
    def _():
        cross(0, hi).start()
        cross(1, hi).start()

    for up, flag in ((True, to_next), (False, to_prev)):

        @pl.when(flag)
        def _(up=up):
            for copy in halo_copies(up):
                copy.start()

    def over(read, weight, columns, width, store):
        @pl.loop(0, columns // width)
        def _(n):
            cols = pl.ds(pl.multiple_of(n * width, width), width)
            store(dot(read(), weight[:, cols]), cols)

    def phase(base, count, waits, ends):
        rows = pl.ds(pl.multiple_of(base, 16), count)
        rows_x = pl.ds(pl.multiple_of(EDGE + base, 16), count)

        def read():
            return tb[rows_x, :]

        def read_x():
            return jnp.concatenate([read(), edge[...]], axis=0) if ends else read()

        def put_x(out, cols):
            out = out.astype(BF).astype(F32)
            xp[rows_x, cols] = out[:count]
            if ends:
                xp[0:EDGE, cols] = out[count : count + EDGE]
                xp[EDGE + TOK :, cols] = out[count + EDGE :]

        def put_bc(out, cols):
            bc[rows, cols] = out.astype(BF)

        if waits:
            loads[4].wait()
        over(read_x, wv, CH, 512, put_x)
        if waits:
            loads[5].wait()
        over(read, ws, 512, 512, put_bc)
        if waits:
            loads[6].wait()
            loads[7].wait()
            loads[8].wait()
            loads[9].wait()
        raw = lax.dot_general(
            read(), wt[...], (((1,), (1,)), ((), ())), preferred_element_type=F32
        ).astype(BF).astype(F32) + par[0:1, :]
        dt_s[rows, :] = jnp.maximum(raw, 0.0) + jnp.log1p(jnp.exp(-jnp.abs(raw)))

    row_i = lax.broadcasted_iota(jnp.int32, (BLK, BLK), 0)
    col_i = lax.broadcasted_iota(jnp.int32, (BLK, BLK), 1)
    lower, upper = row_i >= col_i, col_i >= row_i
    fwd_lane = col_i < 16

    def prepare(j):
        rows = block(j)
        part = dt_s[rows, :] * (par[1:2, :] * -LOG2E)
        high = part.astype(BF)
        rest = part - high.astype(F32)
        mid = rest.astype(BF)
        low = (rest - mid.astype(F32)).astype(BF)
        tri = lower.astype(BF)
        cum = dot(tri, high) + (dot(tri, mid) + dot(tri, low))
        total = cum[BLK - 1 : BLK]
        cum_s[rows, :] = jnp.where(fwd_lane, cum, (total - cum) + part)
        tot_s[pl.ds(j, 1), :] = total

    def scan_in(j, d):
        size = BLK + 2 * EDGE
        rows = block(j)
        fade = jnp.exp2(tot_s[pl.ds(j, 1), :] - cum_s[rows, :]) * dt_s[rows, :]
        bt = bc[rows, d * 256 : d * 256 + 128].astype(F32).T.astype(BF)
        for g in range(8):
            window = xp[block(j, size), lanes(g)]
            acc = None
            for k in range(4):
                o = 3 - k if d else k - 3
                moved = pltpu.roll(window, (-o) % size, 0) if o else window
                term = taps_ref[d, k : k + 1, lanes(g)] * moved[EDGE : EDGE + BLK]
                acc = term if acc is None else acc + term
            x = silu(acc).astype(BF)
            xs[d, rows, lanes(g)] = x
            carried = (x.astype(F32) * expand(fade, d * 16 + 2 * g)).astype(BF)
            upd[d, pl.ds(j, 1), :, lanes(g)] = dot(bt, carried)[None]

    def intra(j):
        rows = block(j)
        cum = cum_s[rows, :]
        cum_t, dt_t = cum.T, dt_s[rows, :].T
        skip = par[2:3, :]
        scores = []
        for d in range(2):
            s = lax.dot_general(
                bc[rows, d * 256 + 128 : d * 256 + 256], bc[rows, d * 256 : d * 256 + 128],
                (((1,), (1,)), ((), ())), preferred_element_type=F32,
            )
            scores.append(jnp.where(lower if d == 0 else upper, s, 0.0))
        for g in range(8):
            values = jnp.concatenate([xs[0, rows, lanes(g)], xs[1, rows, lanes(g)]], axis=0)
            outs = []
            for k in range(2):
                w = []
                for d in range(2):
                    n = d * 16 + 2 * g + k
                    gap = jnp.minimum(cum[:, n : n + 1] - cum_t[n : n + 1, :], 0.0)
                    w.append((scores[d] * jnp.exp2(gap) * dt_t[n : n + 1, :]).astype(BF))
                outs.append(dot(jnp.concatenate(w, axis=1), values))
            y = jnp.where(col_i < 64, outs[0], outs[1])
            for d in range(2):
                y = y + expand(skip, d * 16 + 2 * g) * xs[d, rows, lanes(g)].astype(F32)
            y_s[rows, lanes(g)] = y

    for i in range(1, 4):
        loads[i].wait()
    for i, ref in enumerate((bias_ref, rate_ref, skip_ref)):
        for d in range(2):
            par[i : i + 1, d * 16 : d * 16 + 16] = ref[d : d + 1, :]
    near.wait_recv()

    @pl.when(core != 1 - hi)
    def _():
        cross(0, hi).start()
        cross(1, hi).start()

    cross(2, hi).start()
    cross(3, hi).start()
    phase(hi * HALF, HALF, True, False)
    @pl.when(core == hi)
    def _():
        pass_on(0)

    @pl.when(core != hi)
    def _():
        forwarded(0).wait_recv()

    beside = pl.ds(pl.multiple_of(jnp.where(hi == 0, EDGE + HALF, HALF), 16), EDGE)

    def put_edge(out, cols):
        xp[beside, cols] = out.astype(BF).astype(F32)

    over(lambda: tb[beside, :], wv, CH, 512, put_edge)

    prepare(hi * 2)
    prepare(hi * 2 + 1)
    scan_in(1 + hi, 0)

    @pl.when(core != hi)
    def _():
        pass_on(0)

    pass_on(1)
    scan_in(1 + hi, 1)
    for h in range(2):

        @pl.when(hi == h)
        def _(h=h):
            scan_in(3 * h, 1 - h)

    @pl.when(core == hi)
    def _():
        forwarded(0).wait_recv()

    forwarded(1).wait_recv()
    phase((2 - hi) * BLK, BLK, False, False)
    prepare(2 - hi)
    pass_on(2)
    for h in range(2):

        @pl.when(hi == h)
        def _(h=h):
            scan_in(2 - h, h)

    pass_on(3)
    forwarded(2).wait_recv()
    forwarded(3).wait_recv()
    for up, flag in ((True, first), (False, final)):

        @pl.when(jnp.logical_not(flag))
        def _(up=up):
            halo_copies(up)[0].wait_recv()

    edge[0:16, :] = tb[0:EDGE, :]
    edge[16:32, :] = tb[EDGE + TOK :, :]
    phase((1 - hi) * 3 * BLK, BLK, False, True)
    prepare((1 - hi) * 3)
    for d in range(2):
        scan_in((1 - hi) * 3, d)
    for h in range(2):

        @pl.when(hi == h)
        def _(h=h):
            scan_in(2 - h, 1 - h)
            scan_in(3 * h, h)

    row8 = lax.broadcasted_iota(jnp.int32, (8, 128), 0)
    shrink = jnp.exp2(tot_s[...])
    whole = jnp.exp2(tot_s[0:1, :] + tot_s[1:2, :] + tot_s[2:3, :] + tot_s[3:4, :])
    for g in range(8):
        tail = jnp.zeros((8, 128), F32)
        for d in range(2):
            base = d * 16 + 2 * g
            decay = expand(whole, base)
            high = decay.astype(BF).astype(F32)
            tail = jnp.where(row8 == 2 * d, high, tail)
            tail = jnp.where(row8 == 2 * d + 1, decay - high, tail)
            order = range(NBLK) if d == 0 else range(NBLK - 1, -1, -1)
            state = None
            for j in order:
                new = upd[d, j, :, lanes(g)]
                if state is None:
                    state = new
                else:
                    start[d, j, :, lanes(g)] = state.astype(BF)
                    state = state * expand(shrink[j : j + 1], base) + new
            state = state.astype(BF)
            for r in range(4):
                msg[g * 4 + r, d * 32 : d * 32 + 32] = state[r * 32 : r * 32 + 32]
        for r in range(4):
            msg[g * 4 + r, 64:72] = tail.astype(BF)

    def everywhere(src, dst, send, recv):
        copies = []
        for i, peer in enumerate(peers):
            copy = remote(src.at[peer], dst.at[frame], send.at[i], recv.at[i], dev(peer, row))
            copy.start()
            copies.append(copy)
        dst[frame] = src[frame]
        return copies

    there = everywhere(msg, got, a_s, a_r)

    @pl.loop(0, NBLK)
    def _(i):
        intra(i)

    loads[10].wait()

    def put_gate(out, cols):
        gate[:, cols] = out.astype(BF)

    over(lambda: tb[EDGE : EDGE + TOK, :], wg, CH, 512, put_gate)

    for copy in there:
        copy.wait_recv()
    for d in range(2):
        state = jnp.zeros((32, 128), F32)
        for g in range(FRAMES) if d == 0 else reversed(range(FRAMES)):
            ret[g, d * 32 : d * 32 + 32] = state.astype(BF)
            tail = got[g, 64:72].astype(F32)
            decay = tail[2 * d : 2 * d + 1] + tail[2 * d + 1 : 2 * d + 2]
            state = decay * state + got[g, d * 32 : d * 32 + 32].astype(F32)
    back = everywhere(ret, inc, b_s, b_r)

    def from_start(j, d):
        rows = block(j)
        grown = jnp.exp2(cum_s[rows, :])
        c = bc[rows, d * 256 + 128 : d * 256 + 256]
        for g in range(8):
            y_s[rows, lanes(g)] += expand(grown, d * 16 + 2 * g) * dot(c, start[d, j, :, lanes(g)])

    @pl.loop(0, NBLK - 1)
    def _(i):
        from_start(i + 1, 0)
        from_start(i, 1)

    zero = jnp.zeros((1, 128), F32)
    before, after = [zero], [zero]
    for j in range(NBLK - 1):
        before.append(before[-1] + tot_s[j : j + 1, :])
        after.append(after[-1] + tot_s[NBLK - 1 - j : NBLK - j, :])
    after = after[::-1]
    for j in range(NBLK):
        off_s[j : j + 1, :] = jnp.where(fwd_lane[0:1], before[j], after[j])

    @pl.loop(0, NBLK)
    def _(n):
        target = jnp.where(
            n == 0, corner, jnp.where(n == 1, across, jnp.where(n == 2, partner, row))
        )
        rows = block(target)
        ef = jnp.exp2(cum_s[rows, :] + off_s[pl.ds(target, 1), :])
        for g in range(8):
            open_g = silu(gate[rows, lanes(g)].astype(F32))
            y_s[rows, lanes(g)] = y_s[rows, lanes(g)] * open_g
            for d in range(2):
                ef_s[d, block(n), lanes(g)] = open_g * expand(ef, d * 16 + 2 * g)

    for copy in back:
        copy.wait_recv()
    for g in range(8):
        for r in range(4):
            for d in range(2):
                inc_m[d, r * 32 : r * 32 + 32, lanes(g)] = inc[g * 4 + r, d * 32 : d * 32 + 32]

    def gated_rows(n, target):
        rows = block(target)
        total = jnp.zeros((BLK, BLK), F32)
        for g in range(8):
            gated = y_s[rows, lanes(g)]
            for d in range(2):
                c = bc[rows, d * 256 + 128 : d * 256 + 256]
                gated = gated + ef_s[d, block(n), lanes(g)] * dot(c, inc_m[d, :, lanes(g)])
            total = total + gated * gated
            normed[block(n), lanes(g)] = (gated * gain_ref[:, lanes(g)]).astype(BF)
        sq[n] = jnp.broadcast_to(jnp.sum(total.T, axis=0, keepdims=True), (8, BLK))

    @pl.loop(0, 2)
    def _(n):
        gated_rows(n, jnp.where(n == 0, corner, across))

    loads[11].wait()
    ones, twos, threes = [], [], []

    def relay(k):
        ones[k].wait_recv()
        to_across[k] = (own[k] + from_partner[0, k].astype(F32)).astype(BF)
        copy = remote(
            to_across.at[k], from_across.at[k], f_s.at[NCOL + k], f_r.at[NCOL + k],
            dev(frame, across),
        )
        copy.start()
        twos.append(copy)

    for k in range(NCOL):
        cols = slice(k * COLS, (k + 1) * COLS)
        part = dot(normed[0:HALF, :], wo[:, cols])
        to_partner[0, k] = part[0:BLK].astype(BF)
        copy = remote(
            to_partner.at[0, k], from_partner.at[0, k], f_s.at[k], f_r.at[k], dev(frame, partner)
        )
        copy.start()
        ones.append(copy)
        own[k] = part[BLK:]
        if k >= LAG:
            relay(k - LAG)
    for k in range(NCOL - LAG, NCOL):
        relay(k)
    @pl.loop(2, 4)
    def _(n):
        gated_rows(n, jnp.where(n == 2, partner, row))

    sq_out[0] = sq[0]
    sq_out[1] = sq[2]
    sq_copy = remote(sq_out, sq_part, f_s.at[3 * NCOL], f_r.at[3 * NCOL], dev(frame, partner))
    sq_copy.start()
    for k in range(NCOL):
        cols = slice(k * COLS, (k + 1) * COLS)
        part = dot(normed[HALF:, :], wo[:, cols])
        to_partner[1, k] = part[0:BLK].astype(BF)
        copy = remote(
            to_partner.at[1, k], from_partner.at[1, k], f_s.at[2 * NCOL + k],
            f_r.at[2 * NCOL + k], dev(frame, partner),
        )
        copy.start()
        threes.append(copy)
        own[k] = part[BLK:]
    sq_copy.wait_recv()
    sq_cross[...] = sq[1] + sq_part[0]
    far_copy = remote(
        sq_cross, sq_far, f_s.at[3 * NCOL + 1], f_r.at[3 * NCOL + 1], dev(frame, across)
    )
    far_copy.start()
    for k in range(NCOL):
        threes[k].wait_recv()
        own[k] = own[k] + from_partner[1, k].astype(F32)
    far_copy.wait_recv()
    mean = (sq[3] + sq_part[1] + sq_far[...]) * (1.0 / D_INNER)
    scale = jnp.broadcast_to(lax.rsqrt(mean + 1e-05)[0:1], (BLK, BLK)).T[:, 0:1]
    for k in range(NCOL):
        cols = slice(k * COLS, (k + 1) * COLS)
        twos[k].wait_recv()
        out_ref[:, cols] = (scale * (own[k] + from_across[k].astype(F32))).astype(BF)

    near.wait_send()
    for i in range(CHUNKS):
        cross(i, hi).wait_send()
        forward(i).wait_send()
    for up, flag in ((True, to_next), (False, to_prev)):

        @pl.when(flag)
        def _(up=up):
            for copy in halo_copies(up):
                copy.wait_send()

    for copy in there + back + ones + twos + threes + [sq_copy, far_copy]:
        copy.wait_send()


def layer(*operands):
    dma = pltpu.SemaphoreType.DMA
    vmem = pltpu.VMEM
    return pl.pallas_call(
        layer_body,
        name="layer",
        out_shape=jax.ShapeDtypeStruct((BLK, D), BF),
        in_specs=[ANY] * 11,
        out_specs=VM,
        scratch_shapes=[
            vmem((2, 16), F32), vmem((2, 16), F32), vmem((2, 16), F32), vmem((2, 4, CH), F32),
            vmem((1, CH), F32),
            vmem((TOK + 2 * EDGE, D), BF), vmem((32, D), BF),
            vmem((D, CH), BF), vmem((D, CH), BF), vmem((D, 512), BF), vmem((128, D), BF),
            vmem((CH, D), BF), vmem((8, 128), F32), vmem((TOK, CH), BF), vmem((TOK, 512), BF),
            vmem((TOK + 2 * EDGE, CH), F32),
            vmem((2, TOK, CH), BF),
            vmem((2, NBLK, 128, CH), BF), vmem((2, NBLK, 128, CH), F32), vmem((BLK, CH), BF),
            vmem((TOK, 128), F32), vmem((TOK, 128), F32), vmem((8, 128), F32),
            vmem((TOK, CH), F32), vmem((2, TOK, CH), F32), vmem((8, 128), F32),
            vmem((FRAMES, MSG, 128), BF), vmem((FRAMES, MSG, 128), BF),
            vmem((FRAMES, 64, 128), BF), vmem((FRAMES, 64, 128), BF), vmem((2, 128, CH), BF),
            vmem((TOK, CH), BF), vmem((4, 8, 128), F32),
            vmem((2, NCOL, BLK, COLS), BF), vmem((2, NCOL, BLK, COLS), BF),
            vmem((NCOL, BLK, COLS), BF), vmem((NCOL, BLK, COLS), BF),
            vmem((NCOL, BLK, COLS), F32),
            vmem((2, 8, 128), F32), vmem((2, 8, 128), F32), vmem((8, 128), F32),
            vmem((8, 128), F32),
            dma((12,)), dma((2 * CHUNKS + 9,)), dma((2 * CHUNKS + 3,)),
            dma((PEERS,)), dma((PEERS,)), dma((PEERS,)), dma((PEERS,)),
            dma((3 * NCOL + 2,)), dma((3 * NCOL + 2,)),
        ],
        compiler_params=pltpu.CompilerParams(
            collective_id=0, has_side_effects=True, vmem_limit_bytes=62 * 1024 * 1024
        ),
    )(*operands)


def per_device(
    tokens, w_gate, w_value, w_state_proj, w_step, step_bias, decay_rate, conv_taps,
    skip_gain, norm_gain, w_out,
):
    out = layer(
        tokens[0], w_gate, w_value, w_state_proj, jnp.swapaxes(w_step, 1, 2), w_out,
        step_bias, decay_rate, skip_gain, conv_taps, norm_gain[None, :],
    )
    return out[None]


def solution(mesh):
    in_specs = (
        P("frame", "row", None), P(None, "row"), P(None, "row"), P(), P(None, None, "row"),
        P(None, "row"), P(None, "row"), P(None, None, "row"), P(None, "row"), P("row"),
        P("row", None),
    )
    return jax.shard_map(
        per_device, mesh=mesh, in_specs=in_specs, out_specs=P("frame", "row", None),
        check_vma=False,
    )
```

```python
import jax
import jax.numpy as jnp
from jax import lax
from jax.experimental import pallas as pl
from jax.experimental.pallas import tpu as pltpu
from jax.sharding import PartitionSpec as P

BF = jnp.bfloat16
F32 = jnp.float32
FRAMES = 32
TOK = 512
BLK = 128
NBLK = 4
CH = 1024
D = 2048
HALF = 256
HALO = 8
LOG2E = 1.4426950408889634
D_INNER = 4096
VM = pl.BlockSpec(memory_space=pltpu.VMEM)
ANY = pl.BlockSpec(memory_space=pl.ANY)
MSG = 72


def silu(x):
    return 0.5 * x * (1.0 + jnp.tanh(0.5 * x))


def dot(a, b):
    return jnp.dot(a, b, preferred_element_type=F32)


def dev(frame, row):
    return {"frame": frame, "row": row}


def place():
    frame, row = lax.axis_index("frame"), lax.axis_index("row")
    core = lax.rem(row, 2)
    return frame, row, core, lax.div(row, 2)


def remote(src, dst, send, recv, target):
    return pltpu.make_async_remote_copy(src, dst, send, recv, device_id=target)


CHUNKS = 4
CROWS = 128 // CHUNKS
HALF_BLK = 64
EDGE = 16
COLS = 512
LAG = 1
NCOL = D // COLS
PEERS = FRAMES - 1
STEPS = sorted(
    ((dx, dy, dz) for dx in range(4) for dy in range(4) for dz in range(2) if dx + dy + dz),
    key=lambda s: -(min(s[0], 4 - s[0]) + min(s[1], 4 - s[1]) + s[2]),
)


def expand(values, base):
    lane = lax.broadcasted_iota(jnp.int32, (1, 128), 1)
    return jnp.where(lane < 64, values[:, base : base + 1], values[:, base + 1 : base + 2])


def lanes(group):
    return slice(group * 128, group * 128 + 128)


def block(j, count=BLK, shift=0):
    return pl.ds(pl.multiple_of(j * BLK + shift, 16), count)


def layer_body(
    tok_ref, wg_ref, wv_ref, ws_ref, wt_ref, wo_ref,
    bias_in, rate_in, skip_in, taps_in, gain_in,
    out_ref,
    bias_ref, rate_ref, skip_ref, taps_ref, gain_ref,
    tb, edge, wg, wv, ws, wt, wo, par, gate, bc,
    xp, xs, start, upd, car, cum_s, dt_s, tot_s, y_s, ef_s, off_s,
    msg, got, ret, inc, inc_m,
    normed, sq, to_partner, from_partner, to_across, from_across, own,
    sq_out, sq_part, sq_cross, sq_far,
    w_sem, g_s, g_r, a_s, a_r, b_s, b_r, f_s, f_r,
):
    frame, row, core, hi = place()
    partner = row + 1 - 2 * core
    across = lax.rem(row + 2, 4)
    corner = lax.rem(partner + 2, 4)
    fx, fy, fz = lax.div(frame, 8), lax.rem(lax.div(frame, 2), 4), lax.rem(frame, 2)
    peers = [
        lax.rem(fx + dx, 4) * 8 + lax.rem(fy + dy, 4) * 2 + lax.rem(fz + dz, 2)
        for dx, dy, dz in STEPS
    ]
    first, final = frame == 0, frame == FRAMES - 1

    mine = pl.ds(pl.multiple_of(EDGE + row * BLK, 16), BLK)
    loads = []
    for i, (src, dst) in enumerate((
        (tok_ref, tb.at[mine]), (bias_in, bias_ref), (rate_in, rate_ref), (skip_in, skip_ref),
        (wv_ref, wv), (ws_ref, ws), (wt_ref.at[0], wt.at[0:16]), (wt_ref.at[1], wt.at[16:32]),
        (taps_in, taps_ref), (gain_in, gain_ref), (wg_ref, wg), (wo_ref, wo),
    )):
        copy = pltpu.make_async_copy(src, dst, w_sem.at[i])
        copy.start()
        loads.append(copy)
    tb[0:EDGE, :] = jnp.zeros((EDGE, D), BF)
    tb[EDGE + TOK :, :] = jnp.zeros((EDGE, D), BF)
    barrier = pltpu.get_barrier_semaphore()
    for peer in (partner, across):
        pl.semaphore_signal(barrier, inc=1, device_id=dev(frame, peer))
    for peer in peers:
        pl.semaphore_signal(barrier, inc=1, device_id=dev(peer, row))

    @pl.when(jnp.logical_not(first))
    def _():
        pl.semaphore_signal(barrier, inc=1, device_id=dev(frame - 1, 3))

    @pl.when(jnp.logical_not(final))
    def _():
        pl.semaphore_signal(barrier, inc=1, device_id=dev(frame + 1, 0))

    to_next = jnp.logical_and(row == 3, jnp.logical_not(final))
    to_prev = jnp.logical_and(row == 0, jnp.logical_not(first))
    wt[32:128, :] = jnp.zeros((96, D), BF)
    par[...] = jnp.zeros_like(par)
    loads[0].wait()
    pl.semaphore_wait(
        barrier, 2 + PEERS + jnp.where(jnp.logical_or(to_next, to_prev), 4, 0)
    )

    def chunk_rows(sender, i, side):
        at = jnp.where(side == 1, i % 2, 1 - i % 2) * CROWS + sender * HALF_BLK
        source = 1 + side if i < 2 else 3 * side
        return pl.ds(pl.multiple_of(EDGE + source * BLK + at, 16), CROWS)

    def cross(i, side):
        rows = chunk_rows(core, i, side)
        return remote(tb.at[rows], tb.at[rows], g_s.at[i], g_r.at[i], dev(frame, across))

    def over_chip(i, sender):
        rows = chunk_rows(sender, i, 1 - hi)
        return remote(
            tb.at[rows], tb.at[rows], g_s.at[CHUNKS + i], g_r.at[CHUNKS + i], dev(frame, partner)
        )

    def forward(i):
        return over_chip(i, core)

    def forwarded(i):
        return over_chip(i, 1 - core)

    def pass_on(i):
        cross(i, 1 - hi).wait_recv()
        forward(i).start()

    near = remote(
        tb.at[mine], tb.at[mine], g_s.at[2 * CHUNKS], g_r.at[2 * CHUNKS], dev(frame, partner)
    )

    def halo_copies(up):
        src = tb.at[pl.ds(pl.multiple_of(EDGE + row * BLK + (BLK - HALO if up else 0), HALO), HALO)]
        dst = tb.at[pl.ds(EDGE - HALO if up else EDGE + TOK, HALO)]
        base = 2 * CHUNKS + 1 + (0 if up else 4)
        return [
            remote(
                src, dst, g_s.at[base + r], g_r.at[2 * CHUNKS + 1 + (0 if up else 1)],
                dev(frame + 1 if up else frame - 1, r),
            )
            for r in range(4)
        ]

    near.start()

    @pl.when(core == 1 - hi)
    def _():
        cross(0, hi).start()
        cross(1, hi).start()

    for up, flag in ((True, to_next), (False, to_prev)):

        @pl.when(flag)
        def _(up=up):
            for copy in halo_copies(up):
                copy.start()

    def over(read, weight, columns, width, store):
        @pl.loop(0, columns // width)
        def _(n):
            cols = pl.ds(pl.multiple_of(n * width, width), width)
            store(dot(read(), weight[:, cols]), cols)

    def phase(base, count, waits, ends):
        rows = pl.ds(pl.multiple_of(base, 16), count)
        rows_x = pl.ds(pl.multiple_of(EDGE + base, 16), count)

        def read():
            return tb[rows_x, :]

        def read_x():
            return jnp.concatenate([read(), edge[...]], axis=0) if ends else read()

        def put_x(out, cols):
            out = out.astype(BF).astype(F32)
            xp[rows_x, cols] = out[:count]
            if ends:
                xp[0:EDGE, cols] = out[count : count + EDGE]
                xp[EDGE + TOK :, cols] = out[count + EDGE :]

        def put_bc(out, cols):
            bc[rows, cols] = out.astype(BF)

        if waits:
            loads[4].wait()
        over(read_x, wv, CH, 512, put_x)
        if waits:
            loads[5].wait()
        over(read, ws, 512, 512, put_bc)
        if waits:
            loads[6].wait()
            loads[7].wait()
            loads[8].wait()
            loads[9].wait()
        raw = lax.dot_general(
            read(), wt[...], (((1,), (1,)), ((), ())), preferred_element_type=F32
        ).astype(BF).astype(F32) + par[0:1, :]
        dt_s[rows, :] = jnp.maximum(raw, 0.0) + jnp.log1p(jnp.exp(-jnp.abs(raw)))

    row_i = lax.broadcasted_iota(jnp.int32, (BLK, BLK), 0)
    col_i = lax.broadcasted_iota(jnp.int32, (BLK, BLK), 1)
    lower, upper = row_i >= col_i, col_i >= row_i
    fwd_lane = col_i < 16

    def prepare(j):
        rows = block(j)
        part = dt_s[rows, :] * (par[1:2, :] * -LOG2E)
        high = part.astype(BF)
        rest = part - high.astype(F32)
        mid = rest.astype(BF)
        low = (rest - mid.astype(F32)).astype(BF)
        tri = lower.astype(BF)
        cum = dot(tri, high) + (dot(tri, mid) + dot(tri, low))
        total = cum[BLK - 1 : BLK]
        cum_s[rows, :] = jnp.where(fwd_lane, cum, (total - cum) + part)
        tot_s[pl.ds(j, 1), :] = total

    def scan_in(j, d):
        size = BLK + 2 * EDGE
        rows = block(j)
        fade = jnp.exp2(tot_s[pl.ds(j, 1), :] - cum_s[rows, :]) * dt_s[rows, :]
        bt = bc[rows, d * 256 : d * 256 + 128].astype(F32).T.astype(BF)
        for g in range(8):
            window = xp[block(j, size), lanes(g)]
            acc = None
            for k in range(4):
                o = 3 - k if d else k - 3
                moved = pltpu.roll(window, (-o) % size, 0) if o else window
                term = taps_ref[d, k : k + 1, lanes(g)] * moved[EDGE : EDGE + BLK]
                acc = term if acc is None else acc + term
            x = silu(acc).astype(BF)
            xs[d, rows, lanes(g)] = x
            carried = (x.astype(F32) * expand(fade, d * 16 + 2 * g)).astype(BF)
            upd[d, pl.ds(j, 1), :, lanes(g)] = dot(bt, carried)[None]

    def intra(j):
        rows = block(j)
        cum = cum_s[rows, :]
        cum_t, dt_t = cum.T, dt_s[rows, :].T
        skip = par[2:3, :]
        scores = []
        for d in range(2):
            s = lax.dot_general(
                bc[rows, d * 256 + 128 : d * 256 + 256], bc[rows, d * 256 : d * 256 + 128],
                (((1,), (1,)), ((), ())), preferred_element_type=F32,
            )
            scores.append(jnp.where(lower if d == 0 else upper, s, 0.0))
        for g in range(8):
            values = jnp.concatenate([xs[0, rows, lanes(g)], xs[1, rows, lanes(g)]], axis=0)
            outs = []
            for k in range(2):
                w = []
                for d in range(2):
                    n = d * 16 + 2 * g + k
                    gap = jnp.minimum(cum[:, n : n + 1] - cum_t[n : n + 1, :], 0.0)
                    w.append((scores[d] * jnp.exp2(gap) * dt_t[n : n + 1, :]).astype(BF))
                outs.append(dot(jnp.concatenate(w, axis=1), values))
            y = jnp.where(col_i < 64, outs[0], outs[1])
            for d in range(2):
                y = y + expand(skip, d * 16 + 2 * g) * xs[d, rows, lanes(g)].astype(F32)
            y_s[rows, lanes(g)] = y

    for i in range(1, 4):
        loads[i].wait()
    for i, ref in enumerate((bias_ref, rate_ref, skip_ref)):
        for d in range(2):
            par[i : i + 1, d * 16 : d * 16 + 16] = ref[d : d + 1, :]
    near.wait_recv()

    @pl.when(core != 1 - hi)
    def _():
        cross(0, hi).start()
        cross(1, hi).start()

    cross(2, hi).start()
    cross(3, hi).start()
    phase(hi * HALF, HALF, True, False)
    @pl.when(core == hi)
    def _():
        pass_on(0)

    @pl.when(core != hi)
    def _():
        forwarded(0).wait_recv()

    beside = pl.ds(pl.multiple_of(jnp.where(hi == 0, EDGE + HALF, HALF), 16), EDGE)

    def put_edge(out, cols):
        xp[beside, cols] = out.astype(BF).astype(F32)

    over(lambda: tb[beside, :], wv, CH, 512, put_edge)

    prepare(hi * 2)
    prepare(hi * 2 + 1)
    scan_in(1 + hi, 0)

    @pl.when(core != hi)
    def _():
        pass_on(0)

    pass_on(1)
    scan_in(1 + hi, 1)
    for h in range(2):

        @pl.when(hi == h)
        def _(h=h):
            scan_in(3 * h, 1 - h)

    @pl.when(core == hi)
    def _():
        forwarded(0).wait_recv()

    forwarded(1).wait_recv()
    phase((2 - hi) * BLK, BLK, False, False)
    prepare(2 - hi)
    pass_on(2)
    for h in range(2):

        @pl.when(hi == h)
        def _(h=h):
            scan_in(2 - h, h)

    pass_on(3)
    forwarded(2).wait_recv()
    forwarded(3).wait_recv()
    for up, flag in ((True, first), (False, final)):

        @pl.when(jnp.logical_not(flag))
        def _(up=up):
            halo_copies(up)[0].wait_recv()

    edge[0:16, :] = tb[0:EDGE, :]
    edge[16:32, :] = tb[EDGE + TOK :, :]
    phase((1 - hi) * 3 * BLK, BLK, False, True)
    prepare((1 - hi) * 3)
    for d in range(2):
        scan_in((1 - hi) * 3, d)
    for h in range(2):

        @pl.when(hi == h)
        def _(h=h):
            scan_in(2 - h, 1 - h)
            scan_in(3 * h, h)

    row8 = lax.broadcasted_iota(jnp.int32, (8, 128), 0)
    shrink = jnp.exp2(tot_s[...])
    whole = jnp.exp2(tot_s[0:1, :] + tot_s[1:2, :] + tot_s[2:3, :] + tot_s[3:4, :])
    for g in range(8):
        tail = jnp.zeros((8, 128), F32)
        for d in range(2):
            base = d * 16 + 2 * g
            decay = expand(whole, base)
            high = decay.astype(BF).astype(F32)
            tail = jnp.where(row8 == 2 * d, high, tail)
            tail = jnp.where(row8 == 2 * d + 1, decay - high, tail)
            order = range(NBLK) if d == 0 else range(NBLK - 1, -1, -1)
            state = None
            for j in order:
                new = upd[d, j, :, lanes(g)]
                if state is None:
                    state = new
                else:
                    start[d, j, :, lanes(g)] = state.astype(BF)
                    state = state * expand(shrink[j : j + 1], base) + new
            state = state.astype(BF)
            for r in range(4):
                msg[g * 4 + r, d * 32 : d * 32 + 32] = state[r * 32 : r * 32 + 32]
        for r in range(4):
            msg[g * 4 + r, 64:72] = tail.astype(BF)

    def everywhere(src, dst, send, recv):
        copies = []
        for i, peer in enumerate(peers):
            copy = remote(src.at[peer], dst.at[frame], send.at[i], recv.at[i], dev(peer, row))
            copy.start()
            copies.append(copy)
        dst[frame] = src[frame]
        return copies

    there = everywhere(msg, got, a_s, a_r)

    @pl.loop(0, NBLK)
    def _(i):
        intra(i)

    loads[10].wait()

    def put_gate(out, cols):
        gate[:, cols] = out.astype(BF)

    over(lambda: tb[EDGE : EDGE + TOK, :], wg, CH, 512, put_gate)

    for copy in there:
        copy.wait_recv()
    for d in range(2):
        state = jnp.zeros((32, 128), F32)
        for g in range(FRAMES) if d == 0 else reversed(range(FRAMES)):
            ret[g, d * 32 : d * 32 + 32] = state.astype(BF)
            tail = got[g, 64:72].astype(F32)
            decay = tail[2 * d : 2 * d + 1] + tail[2 * d + 1 : 2 * d + 2]
            state = decay * state + got[g, d * 32 : d * 32 + 32].astype(F32)
    back = everywhere(ret, inc, b_s, b_r)

    def from_start(j, d):
        rows = block(j)
        grown = jnp.exp2(cum_s[rows, :])
        c = bc[rows, d * 256 + 128 : d * 256 + 256]
        for g in range(8):
            y_s[rows, lanes(g)] += expand(grown, d * 16 + 2 * g) * dot(c, start[d, j, :, lanes(g)])

    @pl.loop(0, NBLK - 1)
    def _(i):
        from_start(i + 1, 0)
        from_start(i, 1)

    zero = jnp.zeros((1, 128), F32)
    before, after = [zero], [zero]
    for j in range(NBLK - 1):
        before.append(before[-1] + tot_s[j : j + 1, :])
        after.append(after[-1] + tot_s[NBLK - 1 - j : NBLK - j, :])
    after = after[::-1]
    for j in range(NBLK):
        off_s[j : j + 1, :] = jnp.where(fwd_lane[0:1], before[j], after[j])

    @pl.loop(0, NBLK)
    def _(n):
        target = jnp.where(
            n == 0, corner, jnp.where(n == 1, across, jnp.where(n == 2, partner, row))
        )
        rows = block(target)
        ef = jnp.exp2(cum_s[rows, :] + off_s[pl.ds(target, 1), :])
        for g in range(8):
            open_g = silu(gate[rows, lanes(g)].astype(F32))
            y_s[rows, lanes(g)] = y_s[rows, lanes(g)] * open_g
            for d in range(2):
                ef_s[d, block(n), lanes(g)] = open_g * expand(ef, d * 16 + 2 * g)

    for copy in back:
        copy.wait_recv()
    for g in range(8):
        for r in range(4):
            for d in range(2):
                inc_m[d, r * 32 : r * 32 + 32, lanes(g)] = inc[g * 4 + r, d * 32 : d * 32 + 32]

    def gated_rows(n, target):
        rows = block(target)
        total = jnp.zeros((BLK, BLK), F32)
        for g in range(8):
            gated = y_s[rows, lanes(g)]
            for d in range(2):
                c = bc[rows, d * 256 + 128 : d * 256 + 256]
                gated = gated + ef_s[d, block(n), lanes(g)] * dot(c, inc_m[d, :, lanes(g)])
            total = total + gated * gated
            normed[block(n), lanes(g)] = (gated * gain_ref[:, lanes(g)]).astype(BF)
        sq[n] = jnp.broadcast_to(jnp.sum(total.T, axis=0, keepdims=True), (8, BLK))

    gated_rows(row * 0, corner)
    loads[11].wait()
    ones, twos, threes = [], [], []

    def relay(k):
        ones[k].wait_recv()
        to_across[k] = (own[k] + from_partner[0, k].astype(F32)).astype(BF)
        copy = remote(
            to_across.at[k], from_across.at[k], f_s.at[NCOL + k], f_r.at[NCOL + k],
            dev(frame, across),
        )
        copy.start()
        twos.append(copy)

    def hand_over(k, part):
        to_partner[0, k] = part.astype(BF)
        copy = remote(
            to_partner.at[0, k], from_partner.at[0, k], f_s.at[k], f_r.at[k], dev(frame, partner)
        )
        copy.start()
        ones.append(copy)

    for k in range(NCOL):
        cols = slice(k * COLS, (k + 1) * COLS)
        if k == 0:
            hand_over(k, dot(normed[0:BLK, :], wo[:, cols]))
            gated_rows(row * 0 + 1, across)
            own[k] = dot(normed[BLK:HALF, :], wo[:, cols])
        else:
            part = dot(normed[0:HALF, :], wo[:, cols])
            hand_over(k, part[0:BLK])
            own[k] = part[BLK:]
        if k >= LAG:
            relay(k - LAG)
    for k in range(NCOL - LAG, NCOL):
        relay(k)
    @pl.loop(2, 4)
    def _(n):
        gated_rows(n, jnp.where(n == 2, partner, row))

    sq_out[0] = sq[0]
    sq_out[1] = sq[2]
    sq_copy = remote(sq_out, sq_part, f_s.at[3 * NCOL], f_r.at[3 * NCOL], dev(frame, partner))
    sq_copy.start()
    for k in range(NCOL):
        cols = slice(k * COLS, (k + 1) * COLS)
        part = dot(normed[HALF:, :], wo[:, cols])
        to_partner[1, k] = part[0:BLK].astype(BF)
        copy = remote(
            to_partner.at[1, k], from_partner.at[1, k], f_s.at[2 * NCOL + k],
            f_r.at[2 * NCOL + k], dev(frame, partner),
        )
        copy.start()
        threes.append(copy)
        own[k] = part[BLK:]
    sq_copy.wait_recv()
    sq_cross[...] = sq[1] + sq_part[0]
    far_copy = remote(
        sq_cross, sq_far, f_s.at[3 * NCOL + 1], f_r.at[3 * NCOL + 1], dev(frame, across)
    )
    far_copy.start()
    for k in range(NCOL):
        threes[k].wait_recv()
        own[k] = own[k] + from_partner[1, k].astype(F32)
    far_copy.wait_recv()
    mean = (sq[3] + sq_part[1] + sq_far[...]) * (1.0 / D_INNER)
    scale = jnp.broadcast_to(lax.rsqrt(mean + 1e-05)[0:1], (BLK, BLK)).T[:, 0:1]
    for k in range(NCOL):
        cols = slice(k * COLS, (k + 1) * COLS)
        twos[k].wait_recv()
        out_ref[:, cols] = (scale * (own[k] + from_across[k].astype(F32))).astype(BF)

    near.wait_send()
    for i in range(CHUNKS):
        cross(i, hi).wait_send()
        forward(i).wait_send()
    for up, flag in ((True, to_next), (False, to_prev)):

        @pl.when(flag)
        def _(up=up):
            for copy in halo_copies(up):
                copy.wait_send()

    for copy in there + back + ones + twos + threes + [sq_copy, far_copy]:
        copy.wait_send()


def layer(*operands):
    dma = pltpu.SemaphoreType.DMA
    vmem = pltpu.VMEM
    return pl.pallas_call(
        layer_body,
        name="layer",
        out_shape=jax.ShapeDtypeStruct((BLK, D), BF),
        in_specs=[ANY] * 11,
        out_specs=VM,
        scratch_shapes=[
            vmem((2, 16), F32), vmem((2, 16), F32), vmem((2, 16), F32), vmem((2, 4, CH), F32),
            vmem((1, CH), F32),
            vmem((TOK + 2 * EDGE, D), BF), vmem((32, D), BF),
            vmem((D, CH), BF), vmem((D, CH), BF), vmem((D, 512), BF), vmem((128, D), BF),
            vmem((CH, D), BF), vmem((8, 128), F32), vmem((TOK, CH), BF), vmem((TOK, 512), BF),
            vmem((TOK + 2 * EDGE, CH), F32),
            vmem((2, TOK, CH), BF),
            vmem((2, NBLK, 128, CH), BF), vmem((2, NBLK, 128, CH), F32), vmem((BLK, CH), BF),
            vmem((TOK, 128), F32), vmem((TOK, 128), F32), vmem((8, 128), F32),
            vmem((TOK, CH), F32), vmem((2, TOK, CH), F32), vmem((8, 128), F32),
            vmem((FRAMES, MSG, 128), BF), vmem((FRAMES, MSG, 128), BF),
            vmem((FRAMES, 64, 128), BF), vmem((FRAMES, 64, 128), BF), vmem((2, 128, CH), BF),
            vmem((TOK, CH), BF), vmem((4, 8, 128), F32),
            vmem((2, NCOL, BLK, COLS), BF), vmem((2, NCOL, BLK, COLS), BF),
            vmem((NCOL, BLK, COLS), BF), vmem((NCOL, BLK, COLS), BF),
            vmem((NCOL, BLK, COLS), F32),
            vmem((2, 8, 128), F32), vmem((2, 8, 128), F32), vmem((8, 128), F32),
            vmem((8, 128), F32),
            dma((12,)), dma((2 * CHUNKS + 9,)), dma((2 * CHUNKS + 3,)),
            dma((PEERS,)), dma((PEERS,)), dma((PEERS,)), dma((PEERS,)),
            dma((3 * NCOL + 2,)), dma((3 * NCOL + 2,)),
        ],
        compiler_params=pltpu.CompilerParams(
            collective_id=0, has_side_effects=True, vmem_limit_bytes=62 * 1024 * 1024
        ),
    )(*operands)


def per_device(
    tokens, w_gate, w_value, w_state_proj, w_step, step_bias, decay_rate, conv_taps,
    skip_gain, norm_gain, w_out,
):
    out = layer(
        tokens[0], w_gate, w_value, w_state_proj, jnp.swapaxes(w_step, 1, 2), w_out,
        step_bias, decay_rate, skip_gain, conv_taps, norm_gain[None, :],
    )
    return out[None]


def solution(mesh):
    in_specs = (
        P("frame", "row", None), P(None, "row"), P(None, "row"), P(), P(None, None, "row"),
        P(None, "row"), P(None, "row"), P(None, None, "row"), P(None, "row"), P("row"),
        P("row", None),
    )
    return jax.shard_map(
        per_device, mesh=mesh, in_specs=in_specs, out_specs=P("frame", "row", None),
        check_vma=False,
    )
```
